16 devices in a mesh: dp: 2 (over y, z), fsdp: 8 (over x, core).
Axes of the slice: x: 4, y: 2, z: 1, core: 2. Of those that a mesh axis runs over, the one named last changes fastest.
The devices are a block of a 4x4x8 slice.
Arguments:
- tokens: bfloat16 [256, 128, 2560], P(('dp', 'fsdp')), parts along dimension 0
- gain_in: bfloat16 [2560], P('fsdp')
- w_dq: bfloat16 [2560, 768], P('fsdp')
- gain_q: bfloat16 [768], P('fsdp')
- w_uq: bfloat16 [768, 3840], P('fsdp')
- w_dkv: bfloat16 [2560, 288], P('fsdp')
- gain_kv: bfloat16 [256], P('fsdp')
- w_ukv: bfloat16 [256, 5120], P('fsdp')
- w_out: bfloat16 [2560, 2560], P('fsdp')
Outputs:
- output 1: bfloat16 [256, 128, 2560], P(('dp', 'fsdp')), parts along dimension 0
- output 2: bfloat16 [256, 128, 256], P(('dp', 'fsdp')), parts along dimension 0
- output 3: bfloat16 [256, 128, 32], P(('dp', 'fsdp')), parts along dimension 0
There are 2 independent parts. The reference program is written for one: setup_inputs(seed, part) draws one part's arguments, and reference() takes and returns one part's arrays. A program takes and returns all parts, laid end to end along the dimension named above; an argument that names none is the same for every part.
All inputs are finite; a program needn't handle non-finite values.
Results may differ from the reference program's by a relative error of at most 0.00647724.
Values are sent between devices in bfloat16 or wider.
A program may use at most 768 MiB of HBM per device.

```python
import jax
import jax.numpy as jnp
from jax import lax

PROMPTS = 128
SEQ_LEN = 128
D_MODEL = 2560
N_HEADS = 40
Q_RANK = 768
KV_RANK = 256
NOPE_DIM = 64
ROPE_DIM = 32
V_DIM = 64
EPSILON = 1e-6
ROPE_THETA = 10000.0


def setup_inputs(seed: int = 0, part: int = 0) -> dict:
    key_list = jax.random.split(jax.random.key(seed), 9)

    def draw_weight(sub_key, n_rows, n_cols):
        drawn = jax.random.normal(sub_key, (n_rows, n_cols), jnp.float32) * (n_rows ** -0.5)
        return drawn.astype(jnp.bfloat16)

    def draw_gain(sub_key, n_items, centre):
        drawn = centre * (1.0 + 0.3 * jax.random.normal(sub_key, (n_items,), jnp.float32))
        return drawn.astype(jnp.bfloat16)

    tok_key = jax.random.fold_in(key_list[0], part)
    tokens = jax.random.normal(tok_key, (PROMPTS, SEQ_LEN, D_MODEL), jnp.float32).astype(jnp.bfloat16)
    return {
        'tokens': tokens,
        'gain_in': draw_gain(key_list[1], D_MODEL, 1.0),
        'w_dq': draw_weight(key_list[2], D_MODEL, Q_RANK),
        'gain_q': draw_gain(key_list[3], Q_RANK, 2.0),
        'w_uq': draw_weight(key_list[4], Q_RANK, N_HEADS * (NOPE_DIM + ROPE_DIM)),
        'w_dkv': draw_weight(key_list[5], D_MODEL, KV_RANK + ROPE_DIM),
        'gain_kv': draw_gain(key_list[6], KV_RANK, 1.0),
        'w_ukv': draw_weight(key_list[7], KV_RANK, N_HEADS * (NOPE_DIM + V_DIM)),
        'w_out': draw_weight(key_list[8], N_HEADS * V_DIM, D_MODEL),
    }


def rms_scale(values_in, gain_vec):
    values_f32 = values_in.astype(jnp.float32)
    inv_rms = lax.rsqrt(jnp.mean(values_f32 * values_f32, axis=-1, keepdims=True) + EPSILON)
    return values_f32 * inv_rms * gain_vec.astype(jnp.float32)


def rope_tables():
    half_dim = ROPE_DIM // 2
    inv_freq = ROPE_THETA ** (-2.0 * jnp.arange(half_dim, dtype=jnp.float32) / ROPE_DIM)
    angles = jnp.arange(SEQ_LEN, dtype=jnp.float32)[:, None] * inv_freq[None, :]
    return jnp.cos(angles), jnp.sin(angles)


def apply_rope(values_in, cos_t, sin_t):
    half_dim = values_in.shape[-1] // 2
    lo_half = values_in[..., :half_dim]
    hi_half = values_in[..., half_dim:]
    return jnp.concatenate([lo_half * cos_t - hi_half * sin_t, hi_half * cos_t + lo_half * sin_t], axis=-1)


def one_prompt(tok_rows, gain_in, w_dq, gain_q, w_uq, w_dkv, gain_kv, w_ukv, w_out):
    cos_t, sin_t = rope_tables()
    normed = rms_scale(tok_rows, gain_in).astype(jnp.bfloat16)
    q_down = jnp.dot(normed, w_dq, preferred_element_type=jnp.float32)
    q_lat = rms_scale(q_down, gain_q).astype(jnp.bfloat16)
    q_full = jnp.dot(q_lat, w_uq, preferred_element_type=jnp.float32).reshape(SEQ_LEN, N_HEADS, NOPE_DIM + ROPE_DIM)
    q_nope = q_full[:, :, :NOPE_DIM].astype(jnp.bfloat16)
    q_pe = apply_rope(q_full[:, :, NOPE_DIM:], cos_t[:, None, :], sin_t[:, None, :]).astype(jnp.bfloat16)
    kv_down = jnp.dot(normed, w_dkv, preferred_element_type=jnp.float32)
    latent = rms_scale(kv_down[:, :KV_RANK], gain_kv).astype(jnp.bfloat16)
    k_pe = apply_rope(kv_down[:, KV_RANK:], cos_t, sin_t).astype(jnp.bfloat16)
    kv_up = jnp.dot(latent, w_ukv, preferred_element_type=jnp.float32).astype(jnp.bfloat16)
    kv_up = kv_up.reshape(SEQ_LEN, N_HEADS, NOPE_DIM + V_DIM)
    k_nope = kv_up[:, :, :NOPE_DIM].astype(jnp.float32)
    values = kv_up[:, :, NOPE_DIM:].astype(jnp.float32)
    score_scale = (NOPE_DIM + ROPE_DIM) ** -0.5
    scores = jnp.einsum('qhd,khd->hqk', q_nope.astype(jnp.float32), k_nope)
    scores = scores + jnp.einsum('qhd,kd->hqk', q_pe.astype(jnp.float32), k_pe.astype(jnp.float32))
    causal = jnp.arange(SEQ_LEN)[:, None] >= jnp.arange(SEQ_LEN)[None, :]
    scores = jnp.where(causal[None, :, :], scores * score_scale, -1e30)
    attn_probs = jax.nn.softmax(scores, axis=-1).astype(jnp.bfloat16)
    attn_out = jnp.einsum('hqk,khd->qhd', attn_probs.astype(jnp.float32), values).astype(jnp.bfloat16)
    attn_out = attn_out.reshape(SEQ_LEN, N_HEADS * V_DIM)
    proj_out = jnp.dot(attn_out, w_out, preferred_element_type=jnp.float32)
    y_rows = (tok_rows.astype(jnp.float32) + proj_out).astype(jnp.bfloat16)
    return y_rows, latent, k_pe


def reference(tokens, gain_in, w_dq, gain_q, w_uq, w_dkv, gain_kv, w_ukv, w_out):
    def per_prompt(tok_rows):
        return one_prompt(tok_rows, gain_in, w_dq, gain_q, w_uq, w_dkv, gain_kv, w_ukv, w_out)

    y_out, kv_cache, pe_cache = lax.map(per_prompt, tokens)
    return (y_out, kv_cache, pe_cache)
```

```python
import functools

import jax
import jax.numpy as jnp
import numpy as np
from jax import lax
from jax.experimental import pallas as pl
from jax.experimental.pallas import tpu as pltpu
from jax.sharding import PartitionSpec as P

EPSILON = 1e-6
ROPE_THETA = 10000.0
MESH = pl.DeviceIdType.MESH
BF16 = jnp.bfloat16
F32 = jnp.float32
N_MSG = 14
TILE = 256


def rope_tables(seq_len, rope_dim):
    half_dim = rope_dim // 2
    expo = (-2.0 * np.arange(half_dim, dtype=np.float32) / np.float32(rope_dim)).astype(np.float32)
    inv_freq = np.power(np.float32(ROPE_THETA), expo).astype(np.float32)
    angles = np.arange(seq_len, dtype=np.float32)[:, None] * inv_freq[None, :]
    return np.cos(angles).astype(np.float32), np.sin(angles).astype(np.float32)


def rms(v, gain):
    return v * lax.rsqrt(jnp.mean(v * v, axis=-1, keepdims=True) + EPSILON) * gain


class Item:
    def __init__(self, index, local, full, rows, by_rows, private, col0, cols):
        self.index, self.local, self.full = index, local, full
        self.rows, self.by_rows, self.s = rows, by_rows, private
        self.col0, self.cols = col0, cols
        self.span = rows if by_rows else cols

    def _cut(self, ref, row0, off, size):
        if self.by_rows:
            rows = pl.ds(pl.multiple_of(row0 + off, 16), size)
            cols = pl.ds(self.col0, self.cols)
        else:
            rows = pl.ds(row0 if isinstance(row0, int) else pl.multiple_of(row0, 16), self.rows)
            cols = pl.ds(pl.multiple_of(self.col0 + off, 128), size)
        return ref.at[rows, cols]

    def mine(self, off, size):
        return self._cut(self.local, 0, off, size)

    def at(self, origin, off, size):
        return self._cut(self.full, origin * self.rows, off, size)


def gather_kernel(
    dims, x_hbm, gains_ref, wdq_l, wdkv_l, wuq_l, wukv_l, wo_l, cos_t, sin_t, cos_n, sin_n,
    o_hbm, wo_full, c_hbm, r_hbm,
    gbuf, a_s, wdq, wdkv, acc_q, acc_kv, wuq, wuq_t, wukv, wk, wv_t,
    cq_t, c_s, c_t, r_s, qs, ks, vs, o_s, stage, diff_s,
    ssem, rsem, lsem, gssem, grsem, xsem, osem, csem,
):
    n_dev, n_heads, nope, rope, vdim, d_model, q_rank, kv_rank, seq = dims
    f = lax.axis_index('fsdp')
    d = lax.axis_index('dp')
    core = lax.rem(f, 2)
    par = lax.rem(d, 2)
    chip = f // 2
    n_chip = n_dev // 2
    mod = lambda v: lax.rem(v, n_dev)
    right, left, opp = mod(f + 2), mod(f + n_dev - 2), mod(f + 4)
    partner = f + 1 - 2 * core
    p_right, p_left, p_opp = mod(partner + 2), mod(partner + n_dev - 2), mod(partner + 4)
    d_pair = d + 1 - 2 * par
    to_right, to_left, to_partner, to_pair = (d, right), (d, left), (d, partner), (d_pair, f)
    n_tok = a_s.shape[0]
    n_tile = n_tok // TILE
    half_heads = n_heads // 2
    pairs = half_heads // 2
    hd = nope + rope

    barrier = pltpu.get_barrier_semaphore()
    for step in range(1, n_dev):
        pl.semaphore_signal(barrier, inc=1, device_id=(d, mod(f + step)), device_id_type=MESH)
    pl.semaphore_signal(barrier, inc=1, device_id=to_pair, device_id_type=MESH)
    x_in = [
        pltpu.make_async_copy(x_hbm.at[pl.ds(TILE * t, TILE)], a_s.at[pl.ds(TILE * t, TILE)], xsem.at[t])
        for t in range(n_tile)
    ]
    for cp in x_in:
        cp.start()
    pl.semaphore_wait(barrier, n_dev)

    r_d, r_q, r_kv, r_o = wdq_l.shape[0], wuq_l.shape[0], wukv_l.shape[0], wo_l.shape[0]
    third = lambda n, unit: ((n // unit + 2) // 3) * unit
    items = [
        Item(0, wdq_l, wdq, r_d, True, third(r_d, 16), 0, wdq_l.shape[1]),
        Item(1, wdkv_l, wdkv, r_d, True, third(r_d, 16), 0, wdkv_l.shape[1]),
    ]
    uq_c, ukv_c = wuq_l.shape[1] // 2, wukv_l.shape[1] // 2
    for h in range(2):
        items.append(Item(2 + 2 * h, wuq_l, wuq, r_q, True, third(r_q, 16), h * uq_c, uq_c))
        items.append(Item(3 + 2 * h, wukv_l, wukv, r_kv, False, third(ukv_c, 128), h * ukv_c, ukv_c))
    n_o = 4
    o_c = wo_l.shape[1] // n_o
    for h in range(n_o):
        items.append(Item(6 + h, wo_l, wo_full, r_o, True, third(r_o, 16), h * o_c, o_c))

    def messages(it):
        n, s = it.span, it.s
        own_p, m_off, pm_off, other_p = par * (n - s), s, par * s, (1 - par) * (n - s)
        pm = n - s
        m = n - 2 * s
        reg = it.at
        return [
            (it.mine(pm_off, pm), reg(f, pm_off, pm), to_right, reg(left, pm_off, pm)),
            (it.mine(pm_off, pm), reg(f, pm_off, pm), to_left, reg(right, pm_off, pm)),
            (it.mine(0, n), reg(f, 0, n), to_partner, reg(partner, 0, n)),
            (reg(left, own_p, s), reg(left, own_p, s), to_right, reg(opp, own_p, s)),
            (reg(right, m_off, m), reg(right, m_off, m), to_left, reg(opp, m_off, m)),
            (reg(left, own_p, s), reg(left, own_p, s), to_pair, reg(left, other_p, s)),
            (reg(right, own_p, s), reg(right, own_p, s), to_pair, reg(right, other_p, s)),
            (reg(opp, own_p, s), reg(opp, own_p, s), to_pair, reg(opp, other_p, s)),
            (reg(left, pm_off, pm), reg(left, pm_off, pm), to_partner, reg(p_left, pm_off, pm)),
            (reg(right, pm_off, pm), reg(right, pm_off, pm), to_partner, reg(p_right, pm_off, pm)),
            (reg(opp, pm_off, pm), reg(opp, pm_off, pm), to_partner, reg(p_opp, pm_off, pm)),
            (reg(left, other_p, s), reg(left, other_p, s), to_partner, reg(p_left, other_p, s)),
            (reg(right, other_p, s), reg(right, other_p, s), to_partner, reg(p_right, other_p, s)),
            (reg(opp, other_p, s), reg(opp, other_p, s), to_partner, reg(p_opp, other_p, s)),
        ]

    def send(it, t):
        src, dst, dev, _ = messages(it)[t]
        k = it.index * N_MSG + t
        return pltpu.make_async_remote_copy(src, dst, ssem.at[k], rsem.at[k], device_id=dev, device_id_type=MESH)

    def recv(it, t):
        _, _, dev, got = messages(it)[t]
        k = it.index * N_MSG + t
        return pltpu.make_async_remote_copy(got, got, ssem.at[k], rsem.at[k], device_id=dev, device_id_type=MESH)

    def start(it, *ts):
        for t in ts:
            send(it, t).start()

    def got(it, *ts):
        for t in ts:
            recv(it, t).wait_recv()

    def local_copy(it):
        return pltpu.make_async_copy(it.mine(0, it.span), it.at(f, 0, it.span), lsem.at[it.index])

    stage_in = pltpu.make_async_copy(wo_l, stage, lsem.at[6])
    stage_out = pltpu.make_async_copy(stage, wo_full.at[pl.ds(pl.multiple_of(f * r_o, 16), r_o)], lsem.at[7])

    def step_a(i):
        start(items[i], 0, 1, 2)
        if i < 6:
            local_copy(items[i]).start()

    def step_b(i):
        got(items[i], 0, 1)
        start(items[i], 3, 4, 5, 6, 8, 9)

    def step_c(i):
        got(items[i], 3, 4)
        start(items[i], 7, 10)

    def step_d(i):
        got(items[i], 5, 6)
        start(items[i], 11, 12)

    def step_d2(i):
        got(items[i], 7)
        start(items[i], 13)

    def step_e(i):
        got(items[i], 2, 8, 9, 10, 11, 12, 13)
        if i < 6:
            local_copy(items[i]).wait()

    def gain_copy(step):
        return pltpu.make_async_remote_copy(
            gains_ref, gbuf.at[step - 1], gssem.at[step - 1], grsem.at[step - 1],
            device_id=(d, mod(f + step)), device_id_type=MESH,
        )

    for step in range(1, n_dev):
        gain_copy(step).start()
    step_a(0)
    step_a(1)
    stage_in.start()

    row_i = lax.broadcasted_iota(jnp.int32, (seq, 2 * seq), 0)
    lane_i = lax.broadcasted_iota(jnp.int32, (seq, 2 * seq), 1)
    diff_s[...] = lax.rem(lane_i, seq) - row_i
    for p in range(2):
        @pl.loop(0, pairs)
        def _(j, p=p):
            qs[p, j] = jnp.zeros(qs.shape[2:], BF16)

    @pl.loop(0, pairs)
    def _(j):
        vs[j, 2 * vdim:, :] = jnp.ones((vs.shape[1] - 2 * vdim, vs.shape[2]), BF16)

    r_s[...] = jnp.zeros(r_s.shape, BF16)

    for step in range(1, n_dev):
        gain_copy(step).wait_recv()
    gain = gains_ref[...]
    for step in range(1, n_dev):
        gain = gain + gbuf[step - 1]
    g_in = gain[:, :d_model]
    g_q = gain[:, d_model:d_model + q_rank]
    g_kv = gain[:, d_model + q_rank:]

    for cp in x_in:
        cp.wait()

    @pl.loop(0, n_tok // 64)
    def _(t):
        rows = pl.ds(pl.multiple_of(t * 64, 64), 64)
        a_s[rows, :] = rms(a_s[rows, :].astype(F32), g_in).astype(BF16)

    depth = 2 * r_d

    def down(chip_i, first):
        cols = pl.ds(pl.multiple_of(chip_i * depth, 128), depth)

        @pl.loop(0, n_tile)
        def _(t):
            rows = pl.ds(pl.multiple_of(t * TILE, TILE), TILE)
            a = a_s[rows, cols]
            q = jnp.dot(a, wdq[cols, :], preferred_element_type=F32)
            kv = jnp.dot(a, wdkv[cols, :], preferred_element_type=F32)
            if first:
                acc_q[rows, :] = q
                acc_kv[rows, :] = kv
            else:
                acc_q[rows, :] += q
                acc_kv[rows, :] += kv

    for i in (0, 1):
        got(items[i], 2)
        local_copy(items[i]).wait()
    down(chip, True)
    step_b(0)
    step_b(1)
    step_a(2)
    step_a(3)
    for i in (0, 1):
        step_d(i)
    for i in (0, 1):
        got(items[i], 8, 11)
    down(lax.rem(chip + n_chip - 1, n_chip), False)
    step_c(0)
    step_c(1)
    for i in (0, 1):
        got(items[i], 9, 12)
    down(lax.rem(chip + 1, n_chip), False)
    step_d2(0)
    step_d2(1)
    for i in (0, 1):
        got(items[i], 10, 13)
    down(lax.rem(chip + 2, n_chip), False)
    stage_in.wait()
    stage_out.start()

    @pl.loop(0, n_tile)
    def _(t):
        rows = pl.ds(pl.multiple_of(t * TILE, TILE), TILE)
        cq_t[:, rows] = rms(acc_q[rows, :], g_q).astype(BF16).T
        kv = acc_kv[rows, :]
        lat = rms(kv[:, :kv_rank], g_kv).astype(BF16)
        c_s[rows, :] = lat
        c_t[:, rows] = lat.T
        pe = kv[:, kv_rank:]
        swapped = jnp.concatenate([pe[:, rope // 2:], pe[:, :rope // 2]], axis=1)
        r_s[rows, :rope] = (pe * cos_n[...] + swapped * sin_n[...]).astype(BF16)

    c_out = pltpu.make_async_copy(c_s, c_hbm, csem.at[0])
    r_out = pltpu.make_async_copy(r_s, r_hbm, csem.at[1])
    c_out.start()
    r_out.start()

    step_b(2)
    step_b(3)
    step_a(4)
    step_a(5)
    step_d(2)
    step_d(3)
    step_c(2)
    step_c(3)
    step_d2(2)
    step_d2(3)
    step_e(2)
    step_e(3)

    plan = {
        0: [(step_b, 4), (step_b, 5), (step_a, 6)],
        2: [(step_d, 4), (step_d, 5), (step_c, 4), (step_c, 5)],
        3: [(step_d2, 4), (step_d2, 5)],
        5: [(step_b, 6), (step_a, 7)],
        7: [(step_d, 6), (step_c, 6), (step_e, 4), (step_e, 5)],
        8: [(step_d2, 6)],
        9: [(step_b, 7), (step_a, 8)],
        11: [(step_d, 7), (step_c, 7)],
        12: [(step_d2, 7)],
        13: [(step_b, 8), (step_a, 9)],
        15: [(step_d, 8), (step_c, 8)],
    }
    scale = float((nope + rope) ** -0.5)
    exp_scale = scale * float(np.log2(np.e))
    fill = -1e30 / scale
    cos_q, sin_q = cos_t[...], sin_t[...]
    hr = rope // 2

    def o_copy(slot, t, h):
        return pltpu.make_async_copy(
            o_s.at[slot],
            o_hbm.at[pl.ds(pl.multiple_of(t * TILE, TILE), TILE),
                     pl.ds(pl.multiple_of(h * half_heads * vdim, 128), half_heads * vdim)],
            osem.at[slot],
        )

    chunk = 4

    @pl.loop(0, 2)
    def _(h):
        for b in range(uq_c // 128):
            cols = pl.ds(pl.multiple_of(h * uq_c + b * 128, 128), 128)
            wuq_t[b * 128:(b + 1) * 128, :] = wuq[:, cols].T
        for j in range(pairs):
            c0 = h * ukv_c + j * 2 * (nope + vdim)
            wa = wukv[:, pl.ds(pl.multiple_of(c0, 128), nope + vdim)]
            wb = wukv[:, pl.ds(pl.multiple_of(c0 + nope + vdim, 128), nope + vdim)]
            wk[:, 2 * nope * j:2 * nope * (j + 1)] = jnp.concatenate([wa[:, :nope], wb[:, :nope]], axis=1)
            wv_t[2 * vdim * j:2 * vdim * (j + 1), :] = jnp.concatenate([wa.T[nope:], wb.T[nope:]], axis=0)

        @pl.loop(0, n_tile)
        def _(t):
            it = h * n_tile + t
            for when, todo in plan.items():
                @pl.when(it == when)
                def _(todo=todo):
                    for fn, i in todo:
                        fn(i)
            slot = lax.rem(it, 2)
            rows = pl.ds(pl.multiple_of(t * TILE, TILE), TILE)
            cq = cq_t[:, rows]
            for g in range(half_heads // chunk):
                w = wuq_t[g * chunk * hd:(g + 1) * chunk * hd, :]
                q = jnp.dot(w, cq, preferred_element_type=F32)
                for hh in range(chunk):
                    j, side = (g * chunk + hh) // 2, hh % 2
                    r0 = hh * hd
                    for p in range(2):
                        lanes = slice(seq * p, seq * (p + 1))
                        dst = slice(seq * side, seq * (side + 1))
                        qs[p, j, side * nope:(side + 1) * nope, dst] = q[r0:r0 + nope, lanes].astype(BF16)
                        lo = q[r0 + nope:r0 + nope + hr, lanes]
                        hi = q[r0 + nope + hr:r0 + hd, lanes]
                        qs[p, j, 2 * nope:2 * nope + hr, dst] = (lo * cos_q - hi * sin_q).astype(BF16)
                        qs[p, j, 2 * nope + hr:2 * nope + rope, dst] = (hi * cos_q + lo * sin_q).astype(BF16)
            lat = c_s[rows, :]
            ks[...] = jnp.dot(lat, wk[...], preferred_element_type=F32).astype(BF16)
            v = jnp.dot(wv_t[...], c_t[:, rows], preferred_element_type=F32).astype(BF16)
            for j in range(pairs):
                vs[j, :2 * vdim, :] = v[2 * vdim * j:2 * vdim * (j + 1)]

            @pl.when(it >= 2)
            def _():
                o_copy(slot, t, h).wait()

            for p in range(2):
                r_blk = r_s[pl.ds(pl.multiple_of(t * TILE + p * seq, seq), seq), :]
                for j in range(pairs):
                    lhs = jnp.concatenate([ks[seq * p:seq * (p + 1), 2 * nope * j:2 * nope * (j + 1)], r_blk], axis=1)
                    s = jnp.dot(lhs, qs[p, j], preferred_element_type=F32)
                    s = jnp.where(diff_s[...] >= 0, s, fill)
                    m = jnp.max(s, axis=0, keepdims=True)
                    e = jnp.exp2((s - m) * exp_scale).astype(BF16)
                    ov = jnp.dot(vs[j, :, seq * p:seq * (p + 1)], e, preferred_element_type=F32)
                    inv = 1.0 / ov[2 * vdim:2 * vdim + 1, :]
                    oa = ov[:vdim, :seq] * inv[:, :seq]
                    ob = ov[vdim:2 * vdim, seq:] * inv[:, seq:]
                    o_t = jnp.concatenate([oa, ob], axis=0).astype(BF16)
                    o_s[slot, seq * p:seq * (p + 1), 2 * vdim * j:2 * vdim * (j + 1)] = o_t.T
            o_copy(slot, t, h).start()

    step_d2(8)
    step_b(9)
    step_d(9)
    step_c(9)
    step_d2(9)
    for i in range(6, 6 + n_o):
        step_e(i)
    stage_out.wait()
    o_copy(0, n_tile - 2, 1).wait()
    o_copy(1, n_tile - 1, 1).wait()
    c_out.wait()
    r_out.wait()
    for step in range(1, n_dev):
        gain_copy(step).wait_send()
    for it in items:
        for t in range(N_MSG):
            send(it, t).wait_send()


def out_kernel(o_ref, w_ref, x_ref, c_ref, r_ref, y_ref, c_out, r_out):
    acc = jnp.dot(o_ref[...], w_ref[...], preferred_element_type=F32)
    y_ref[...] = (x_ref[...].astype(F32) + acc).astype(BF16)
    c_out[...] = c_ref[...]
    r_out[...] = r_ref[:, :r_out.shape[1]]


def solution(mesh):
    batch_spec = P(('dp', 'fsdp'))
    row_spec = P('fsdp')
    mat_spec = P('fsdp', None)
    n_dev = mesh.shape['fsdp']
    assert n_dev == 8 and mesh.shape['dp'] % 2 == 0

    def local_block(tok, g_in, w_dq, g_q, w_uq, w_dkv, g_kv, w_ukv, w_out):
        n_p, seq, d_model = tok.shape
        n_tok = n_p * seq
        kv_rank, q_rank = g_kv.shape[0] * n_dev, g_q.shape[0] * n_dev
        rope = w_dkv.shape[1] - kv_rank
        nope_total = w_ukv.shape[1] - w_out.shape[0] * n_dev
        n_heads = (w_uq.shape[1] - nope_total) // rope
        nope = nope_total // n_heads
        vdim = w_out.shape[0] * n_dev // n_heads
        pairs = n_heads // 4
        hh = n_heads // 2
        x2 = tok.reshape(n_tok, d_model)
        me = lax.axis_index('fsdp')

        def spread(g, total):
            return lax.dynamic_update_slice(jnp.zeros((total,), F32), g.astype(F32), (me * g.shape[0],))

        gains = jnp.concatenate([spread(g_in, d_model), spread(g_q, q_rank), spread(g_kv, kv_rank)])[None]
        cos, sin = rope_tables(seq, rope)
        cos_t, sin_t = jnp.asarray(cos.T), jnp.asarray(sin.T)
        reps = TILE // seq
        cos_n = jnp.asarray(np.tile(np.concatenate([cos, cos], 1), (reps, 1)))
        sin_n = jnp.asarray(np.tile(np.concatenate([-sin, sin], 1), (reps, 1)))
        dims = (n_dev, n_heads, nope, rope, vdim, d_model, q_rank, kv_rank, seq)
        n_items = 10
        any_ = pl.BlockSpec(memory_space=pl.ANY)
        vm = pl.BlockSpec(memory_space=pltpu.VMEM)
        o, wo_full, c_all, r_all = pl.pallas_call(
            functools.partial(gather_kernel, dims),
            out_shape=(
                jax.ShapeDtypeStruct((n_tok, n_heads * vdim), BF16),
                jax.ShapeDtypeStruct((n_heads * vdim, d_model), BF16),
                jax.ShapeDtypeStruct((n_tok, kv_rank), BF16),
                jax.ShapeDtypeStruct((n_tok, 128), BF16),
            ),
            in_specs=[any_, vm] + [any_] * 5 + [vm] * 4,
            out_specs=(any_,) * 4,
            scratch_shapes=[
                pltpu.VMEM((n_dev - 1, 1, gains.shape[1]), F32),
                pltpu.VMEM((n_tok, d_model), BF16),
                pltpu.VMEM((d_model, q_rank), BF16),
                pltpu.VMEM((d_model, kv_rank + rope), BF16),
                pltpu.VMEM((n_tok, q_rank), F32),
                pltpu.VMEM((n_tok, kv_rank + rope), F32),
                pltpu.VMEM((q_rank, w_uq.shape[1]), BF16),
                pltpu.VMEM((w_uq.shape[1] // 2, q_rank), BF16),
                pltpu.VMEM((kv_rank, w_ukv.shape[1]), BF16),
                pltpu.VMEM((kv_rank, hh * nope), BF16),
                pltpu.VMEM((hh * vdim, kv_rank), BF16),
                pltpu.VMEM((q_rank, n_tok), BF16),
                pltpu.VMEM((n_tok, kv_rank), BF16),
                pltpu.VMEM((kv_rank, n_tok), BF16),
                pltpu.VMEM((n_tok, 128), BF16),
                pltpu.VMEM((2, pairs, 2 * nope + 128, 2 * seq), BF16),
                pltpu.VMEM((TILE, hh * nope), BF16),
                pltpu.VMEM((pairs, 2 * vdim + 16, TILE), BF16),
                pltpu.VMEM((2, TILE, hh * vdim), BF16),
                pltpu.VMEM(w_out.shape, BF16),
                pltpu.VMEM((seq, 2 * seq), jnp.int32),
                pltpu.SemaphoreType.DMA((n_items * N_MSG,)),
                pltpu.SemaphoreType.DMA((n_items * N_MSG,)),
                pltpu.SemaphoreType.DMA((8,)),
                pltpu.SemaphoreType.DMA((n_dev - 1,)),
                pltpu.SemaphoreType.DMA((n_dev - 1,)),
                pltpu.SemaphoreType.DMA((n_tok // TILE,)),
                pltpu.SemaphoreType.DMA((2,)),
                pltpu.SemaphoreType.DMA((2,)),
            ],
            compiler_params=pltpu.CompilerParams(
                collective_id=0, has_side_effects=True, vmem_limit_bytes=67_043_328
            ),
            name='gather_attend',
        )(x2, gains, w_dq, w_dkv, w_uq, w_ukv, w_out, cos_t, sin_t, cos_n, sin_n)

        bm, bn = 512, 512
        n_m, n_n = n_tok // bm, d_model // bn
        once = lambda n, m: (jnp.where(n == 0, m, n_m - 1), 0)
        y, c_blk, r_blk = pl.pallas_call(
            out_kernel,
            grid=(n_n, n_m),
            in_specs=[
                pl.BlockSpec((bm, n_heads * vdim), lambda n, m: (m, 0)),
                pl.BlockSpec((n_heads * vdim, bn), lambda n, m: (0, n)),
                pl.BlockSpec((bm, bn), lambda n, m: (m, n)),
                pl.BlockSpec((bm, kv_rank), once),
                pl.BlockSpec((bm, 128), once),
            ],
            out_specs=[
                pl.BlockSpec((bm, bn), lambda n, m: (m, n)),
                pl.BlockSpec((bm, kv_rank), once),
                pl.BlockSpec((bm, rope), once),
            ],
            out_shape=[
                jax.ShapeDtypeStruct((n_tok, d_model), BF16),
                jax.ShapeDtypeStruct((n_tok, kv_rank), BF16),
                jax.ShapeDtypeStruct((n_tok, rope), BF16),
            ],
            compiler_params=pltpu.CompilerParams(vmem_limit_bytes=48 * 1024 * 1024),
            name='project_out',
        )(o, wo_full, x2, c_all, r_all)
        return y.reshape(tok.shape), c_blk.reshape(n_p, seq, kv_rank), r_blk.reshape(n_p, seq, rope)

    return jax.shard_map(
        local_block,
        mesh=mesh,
        in_specs=(batch_spec, row_spec, mat_spec, row_spec, mat_spec, mat_spec, row_spec, mat_spec, mat_spec),
        out_specs=(batch_spec, batch_spec, batch_spec),
        check_vma=False,
    )
```

```python
import functools

import jax
import jax.numpy as jnp
import numpy as np
from jax import lax
from jax.experimental import pallas as pl
from jax.experimental.pallas import tpu as pltpu
from jax.sharding import PartitionSpec as P

EPSILON = 1e-6
ROPE_THETA = 10000.0
MESH = pl.DeviceIdType.MESH
BF16 = jnp.bfloat16
F32 = jnp.float32
N_MSG = 14
TILE = 256
NORM = 128


def rope_tables(seq_len, rope_dim):
    half_dim = rope_dim // 2
    expo = (-2.0 * np.arange(half_dim, dtype=np.float32) / np.float32(rope_dim)).astype(np.float32)
    inv_freq = np.power(np.float32(ROPE_THETA), expo).astype(np.float32)
    angles = np.arange(seq_len, dtype=np.float32)[:, None] * inv_freq[None, :]
    return np.cos(angles).astype(np.float32), np.sin(angles).astype(np.float32)


def rms(v, gain):
    return v * lax.rsqrt(jnp.mean(v * v, axis=-1, keepdims=True) + EPSILON) * gain


THEN = {0: (3, 5, 8), 1: (4, 6, 9), 3: (7,), 4: (10,), 5: (11,), 6: (12,), 7: (13,)}
ROUTE = 'RLDRLZZZDDDDDD'
SPLITS = ((112, 160), (32, 48), (64, 128), (32, 32), (512, 768), (32, 48), (896, 896),
          (96, 128), (80, 112), (96, 112), (48, 80))
T_NORM, T_DOWN, T_PREP, T_ITER = 6.0, 2.6, 1.9, 2.7


def plan_transfers(pieces, steps):
    rate = {'R': 46.6e3, 'L': 46.6e3, 'Z': 46.6e3, 'D': 300e3}
    hop = {'R': 2.3, 'L': 2.3, 'Z': 2.3, 'D': 1.5}
    free = dict.fromkeys(rate, 0.0)
    state = {'now': 2.5, 'next': 0}
    arrival, done, lists = {}, set(), []

    def send(i, t):
        n, p, r, unit = pieces[i]
        pm = n - p
        size = (pm, pm, n, r, pm - r, p, p, p, pm, pm, pm, p, p, p)[t] * unit
        link = ROUTE[t]
        free[link] = max(state['now'], free[link]) + size / rate[link]
        arrival[i, t] = free[link] + hop[link]

    def own(out):
        i = state['next']
        state['next'] = i + 1
        for t in (0, 1, 2):
            send(i, t)
        out.append((i, -1))

    def wait(i, t, out):
        state['now'] = max(state['now'], arrival[i, t])
        done.add((i, t))
        out.append((i, t))
        for u in THEN.get(t, ()):
            send(i, u)

    for k, (need, busy) in enumerate(steps):
        out = []
        while True:
            while state['next'] < len(pieces) and (
                k == 0 and state['next'] < 3 or min(free['R'], free['L']) - state['now'] < 4
            ):
                own(out)
            ready = sorted(
                (a, i, t) for (i, t), a in arrival.items()
                if (i, t) not in done and t in THEN and (t != 4 or (i, 3) in done)
            )
            if ready and ready[0][0] + 0.3 <= state['now']:
                wait(*ready[0][1:], out)
                continue
            missing = [m for m in need if m not in done]
            if not missing:
                break
            here = [m for m in missing if m in arrival and arrival[m] <= state['now']]
            if here:
                wait(*here[0], out)
                continue
            ready += [(arrival[m], *m) for m in missing if m in arrival and m[1] not in THEN]
            wait(*min(ready)[1:], out)
        lists.append(out)
        state['now'] += busy
    return lists


class Item:
    def __init__(self, index, local, full, rows, by_rows, split, col0, cols):
        self.index, self.local, self.full = index, local, full
        self.rows, self.by_rows = rows, by_rows
        self.s, self.h = split
        self.col0, self.cols = col0, cols
        self.span = rows if by_rows else cols

    def _cut(self, ref, row0, off, size):
        if self.by_rows:
            rows = pl.ds(pl.multiple_of(row0 + off, 16), size)
            cols = pl.ds(self.col0, self.cols)
        else:
            rows = pl.ds(row0 if isinstance(row0, int) else pl.multiple_of(row0, 16), self.rows)
            cols = pl.ds(pl.multiple_of(self.col0 + off, 128), size)
        return ref.at[rows, cols]

    def mine(self, off, size):
        return self._cut(self.local, 0, off, size)

    def at(self, origin, off, size):
        return self._cut(self.full, origin * self.rows, off, size)


def gather_kernel(
    dims, x_hbm, gains_hbm, wdq_l, wdkv_l, wuq_l, wukv_l, wo_l, cos_t, sin_t, cos_n, sin_n,
    o_hbm, wo_full, c_hbm, r_hbm,
    gbuf, a_s, wdq, wdkv, acc_q, acc_kv, wuq, wuq_t, wukv, wk, wv_t,
    cq_t, c_s, c_t, r_s, qs, ks, vs, o_s, stage, diff_s, inv_s, gb_s, s_buf, pm, ms,
    ssem, rsem, lsem, gssem, grsem, xsem, osem, csem,
):
    n_dev, n_heads, nope, rope, vdim, d_model, q_rank, kv_rank, seq = dims
    f = lax.axis_index('fsdp')
    d = lax.axis_index('dp')
    core = lax.rem(f, 2)
    par = lax.rem(d, 2)
    chip = f // 2
    n_chip = n_dev // 2
    mod = lambda v: lax.rem(v, n_dev)
    right, left, opp = mod(f + 2), mod(f + n_dev - 2), mod(f + 4)
    partner = f + 1 - 2 * core
    p_right, p_left, p_opp = mod(partner + 2), mod(partner + n_dev - 2), mod(partner + 4)
    d_pair = d + 1 - 2 * par
    to_right, to_left, to_partner, to_pair = (d, right), (d, left), (d, partner), (d_pair, f)
    n_tok = a_s.shape[0]
    n_tile = n_tok // TILE
    half_heads = n_heads // 2
    pairs = half_heads // 2
    hd = nope + rope

    barrier = pltpu.get_barrier_semaphore()
    for step in range(1, n_dev):
        pl.semaphore_signal(barrier, inc=1, device_id=(d, mod(f + step)), device_id_type=MESH)
    pl.semaphore_signal(barrier, inc=1, device_id=to_pair, device_id_type=MESH)
    x_in = [
        pltpu.make_async_copy(x_hbm.at[pl.ds(TILE * t, TILE)], a_s.at[pl.ds(TILE * t, TILE)], xsem.at[t])
        for t in range(n_tile)
    ]
    for cp in x_in:
        cp.start()
    gain_in = pltpu.make_async_copy(gains_hbm, gbuf.at[f], lsem.at[9])
    gain_in.start()
    pl.semaphore_wait(barrier, n_dev)

    r_d, r_q, r_kv, r_o = wdq_l.shape[0], wuq_l.shape[0], wukv_l.shape[0], wo_l.shape[0]
    n_d, n_o = 2, 4
    dq_c, uq_c, ukv_c, o_c = wdq_l.shape[1] // n_d, wuq_l.shape[1] // 2, wukv_l.shape[1] // 2, wo_l.shape[1] // n_o
    parts = [(wdq_l, wdq, r_d, True, h * dq_c, dq_c) for h in range(n_d)]
    parts.append((wdkv_l, wdkv, r_d, True, 0, wdkv_l.shape[1]))
    n_down = len(parts)
    for h in range(2):
        parts.append((wuq_l, wuq, r_q, True, h * uq_c, uq_c))
        parts.append((wukv_l, wukv, r_kv, False, h * ukv_c, ukv_c))
    n_head = len(parts)
    parts += [(wo_l, wo_full, r_o, True, h * o_c, o_c) for h in range(n_o)]
    items = [Item(k, *p[:4], SPLITS[k], *p[4:]) for k, p in enumerate(parts)]

    everything = range(N_MSG)
    needs = lambda lo, hi, ts=everything: [(i, t) for i in range(lo, hi) for t in ts]
    steps = [([], T_NORM), ([], T_NORM)]
    steps += [(needs(0, n_down, (2,)), T_DOWN), ([], T_DOWN)]
    steps += [(needs(0, n_down, (0, 1, 5, 6, 8, 9, 11, 12)), 2 * T_DOWN), ([], 2 * T_DOWN)]
    steps += [(needs(0, n_down), 1.2 * T_DOWN), ([], 1.2 * T_DOWN)]
    first_iter = len(steps) + 1
    for h in range(2):
        for t in range(n_tile):
            need = needs(n_down + 2 * h, n_down + 2 * h + 2) if t == 0 else []
            steps.append((need, T_ITER + (T_PREP if t == 0 else 0)))
    steps.append((needs(n_head, len(parts)), 0))
    pieces = [
        (it.span, it.s, it.h, 2 * (-(-it.cols // 128) * 128 if it.by_rows else it.rows)) for it in items
    ]
    plan = plan_transfers(pieces, [([], 0)] + steps)

    def messages(it):
        n, s, h = it.span, it.s, it.h
        own_p, pm_off, other_p = par * (n - s), par * s, (1 - par) * (n - s)
        pm, m = n - s, n - s - h
        h_off, m_off = par * (n - h), (1 - par) * h + par * s
        reg = it.at
        return [
            (it.mine(pm_off, pm), reg(f, pm_off, pm), to_right, reg(left, pm_off, pm)),
            (it.mine(pm_off, pm), reg(f, pm_off, pm), to_left, reg(right, pm_off, pm)),
            (it.mine(0, n), reg(f, 0, n), to_partner, reg(partner, 0, n)),
            (reg(left, h_off, h), reg(left, h_off, h), to_right, reg(opp, h_off, h)),
            (reg(right, m_off, m), reg(right, m_off, m), to_left, reg(opp, m_off, m)),
            (reg(left, own_p, s), reg(left, own_p, s), to_pair, reg(left, other_p, s)),
            (reg(right, own_p, s), reg(right, own_p, s), to_pair, reg(right, other_p, s)),
            (reg(opp, own_p, s), reg(opp, own_p, s), to_pair, reg(opp, other_p, s)),
            (reg(left, pm_off, pm), reg(left, pm_off, pm), to_partner, reg(p_left, pm_off, pm)),
            (reg(right, pm_off, pm), reg(right, pm_off, pm), to_partner, reg(p_right, pm_off, pm)),
            (reg(opp, pm_off, pm), reg(opp, pm_off, pm), to_partner, reg(p_opp, pm_off, pm)),
            (reg(left, other_p, s), reg(left, other_p, s), to_partner, reg(p_left, other_p, s)),
            (reg(right, other_p, s), reg(right, other_p, s), to_partner, reg(p_right, other_p, s)),
            (reg(opp, other_p, s), reg(opp, other_p, s), to_partner, reg(p_opp, other_p, s)),
        ]

    def send(it, t):
        src, dst, dev, _ = messages(it)[t]
        k = it.index * N_MSG + t
        return pltpu.make_async_remote_copy(src, dst, ssem.at[k], rsem.at[k], device_id=dev, device_id_type=MESH)

    def recv(it, t):
        _, _, dev, got = messages(it)[t]
        k = it.index * N_MSG + t
        return pltpu.make_async_remote_copy(got, got, ssem.at[k], rsem.at[k], device_id=dev, device_id_type=MESH)

    def start(it, *ts):
        for t in ts:
            send(it, t).start()

    def got(it, *ts):
        for t in ts:
            recv(it, t).wait_recv()

    def local_copy(it):
        return pltpu.make_async_copy(it.mine(0, it.span), it.at(f, 0, it.span), lsem.at[it.index])

    stage_in = pltpu.make_async_copy(wo_l, stage, lsem.at[n_head])
    stage_out = pltpu.make_async_copy(stage, wo_full.at[pl.ds(pl.multiple_of(f * r_o, 16), r_o)], lsem.at[n_head + 1])

    def pump(segment):
        for i, t in segment:
            it = items[i]
            if t < 0:
                start(it, 0, 1, 2)
                if i < n_head:
                    local_copy(it).start()
            else:
                got(it, t)
                start(it, *THEN.get(t, ()))

    def own_rows(first, last):
        for i in range(first, last):
            local_copy(items[i]).wait()

    def gain_copy(step):
        return pltpu.make_async_remote_copy(
            gbuf.at[f], gbuf.at[f], gssem.at[step - 1], grsem.at[step - 1],
            device_id=(d, mod(f + step)), device_id_type=MESH,
        )

    gain_in.wait()
    for step in range(1, n_dev):
        gain_copy(step).start()
    pump(plan[0])
    stage_in.start()

    row_i = lax.broadcasted_iota(jnp.int32, (seq, 2 * seq), 0)
    lane_i = lax.broadcasted_iota(jnp.int32, (seq, 2 * seq), 1)
    diff_s[...] = lax.rem(lane_i, seq) - row_i
    for p in range(2):
        @pl.loop(0, pairs)
        def _(j, p=p):
            qs[p, j] = jnp.zeros(qs.shape[2:], BF16)

    @pl.loop(0, pairs)
    def _(j):
        for b in range(2):
            vs[b, j, :2 * vdim, :] = jnp.zeros((2 * vdim, vs.shape[3]), BF16)
            vs[b, j, 2 * vdim:, :] = jnp.ones((vs.shape[2] - 2 * vdim, vs.shape[3]), BF16)
        s_buf[1, j] = jnp.zeros(s_buf.shape[2:], F32)

    r_s[...] = jnp.zeros(r_s.shape, BF16)
    ms[...] = jnp.zeros(ms.shape, F32)

    for t, cp in enumerate(x_in):
        cp.wait()
        v = a_s[TILE * t:TILE * (t + 1), :].astype(F32)
        inv_s[TILE * t:TILE * (t + 1), :] = lax.rsqrt(jnp.mean(v * v, axis=-1, keepdims=True) + EPSILON)

    for step in range(1, n_dev):
        gain_copy(step).wait_recv()
    n_in, n_q, n_kv = d_model // n_dev, q_rank // n_dev, kv_rank // n_dev
    join = lambda lo, n: jnp.concatenate([gbuf[i][:, lo:lo + n] for i in range(n_dev)], axis=1)
    g_in, g_q, g_kv = join(0, n_in), join(n_in, n_q), join(n_in + n_q, n_kv)

    gb_s[...] = jnp.broadcast_to(g_in, gb_s.shape)
    pump(plan[1])

    @pl.loop(0, n_tok // NORM)
    def _(t):
        rows = pl.ds(pl.multiple_of(t * NORM, NORM), NORM)
        v = a_s[rows, :].astype(F32) * inv_s[rows, :]
        v = v.reshape(NORM // 8, 8, d_model) * gb_s[...][None]
        a_s[rows, :] = v.reshape(NORM, d_model).astype(BF16)

    pump(plan[2])

    depth = 2 * r_d

    chip_cols = lambda c: pl.ds(pl.multiple_of(lax.rem(chip + c, n_chip) * depth, 128), depth)
    tile_rows = lambda t: pl.ds(pl.multiple_of(t * TILE, TILE), TILE)

    def down(t, hops):
        rows = tile_rows(t)
        cols = [chip_cols(c) for c in hops]
        a = jnp.concatenate([a_s[rows, c] for c in cols], axis=1)
        for w, acc in ((wdq, acc_q), (wdkv, acc_kv)):
            part = jnp.dot(a, jnp.concatenate([w[c, :] for c in cols], axis=0), preferred_element_type=F32)
            if hops[0] == 0:
                acc[rows, :] = part
            else:
                acc[rows, :] += part

    def finish(t):
        rows = tile_rows(t)
        cq_t[:, rows] = rms(acc_q[rows, :], g_q).astype(BF16).T
        kv = acc_kv[rows, :]
        lat = rms(kv[:, :kv_rank], g_kv).astype(BF16)
        c_s[rows, :] = lat
        c_t[:, rows] = lat.T
        pe = kv[:, kv_rank:]
        swapped = jnp.concatenate([pe[:, rope // 2:], pe[:, :rope // 2]], axis=1)
        r_s[rows, :rope] = (pe * cos_n[...] + swapped * sin_n[...]).astype(BF16)

    own_rows(0, n_down)
    for k, hops in enumerate(((0,), (n_chip - 1, 1))):
        pump(plan[3 + 2 * k])

        @pl.loop(0, n_tile)
        def _(t):
            @pl.when(t == n_tile // 2)
            def _():
                pump(plan[4 + 2 * k])
            down(t, hops)

    pump(plan[7])
    down(0, (2,))

    @pl.loop(1, n_tile)
    def _(t):
        @pl.when(t == n_tile // 2)
        def _():
            pump(plan[8])
        down(t, (2,))
        finish(t - 1)

    finish(n_tile - 1)
    stage_in.wait()
    stage_out.start()
    c_out = pltpu.make_async_copy(c_s, c_hbm, csem.at[0])
    r_out = pltpu.make_async_copy(r_s, r_hbm, csem.at[1])
    c_out.start()
    r_out.start()

    scale = float((nope + rope) ** -0.5)
    exp_scale = scale * float(np.log2(np.e))
    fill = -1e30 / scale
    cos_q, sin_q = cos_t[...], sin_t[...]
    hr = rope // 2

    def o_copy(it):
        h, t, slot = it // n_tile, it % n_tile, it % 3
        return pltpu.make_async_copy(
            o_s.at[slot],
            o_hbm.at[pl.ds(pl.multiple_of(t * TILE, TILE), TILE),
                     pl.ds(pl.multiple_of(h * half_heads * vdim, 128), half_heads * vdim)],
            osem.at[slot],
        )

    groups = seq // 8

    def maxima(p):
        for side in range(2):
            base = 16 * pairs * side + 8 * pairs * p
            part = [pm[pl.ds(base + i, pairs, stride=8), :] for i in range(8)]
            ms[pairs * p:pairs * (p + 1), seq * side:seq * (side + 1)] = functools.reduce(jnp.maximum, part)

    def values(p, j, slot, o_slot):
        k = p * pairs + j
        m = jnp.broadcast_to(ms[k:k + 1, :], (8, 2 * seq))
        s = s_buf[p, j].reshape(groups, 8, 2 * seq)
        e = jnp.exp2((s - m[None]) * exp_scale).astype(BF16).reshape(seq, 2 * seq)
        ov = jnp.dot(vs[slot, j, :, seq * p:seq * (p + 1)], e, preferred_element_type=F32)
        inv = (1.0 / ov[2 * vdim:2 * vdim + 8, :])[None]
        oa = ov[:vdim, :seq].reshape(vdim // 8, 8, seq) * inv[:, :, :seq]
        ob = ov[vdim:2 * vdim, seq:].reshape(vdim // 8, 8, seq) * inv[:, :, seq:]
        o_t = jnp.concatenate([oa, ob], axis=0).reshape(2 * vdim, seq).astype(BF16)
        o_s[o_slot, seq * p:seq * (p + 1), 2 * vdim * j:2 * vdim * (j + 1)] = o_t.T

    chunk = 4

    @pl.loop(0, 2)
    def _(h):
        for k in range(2):
            @pl.when(h == k)
            def _(k=k):
                pump(plan[first_iter + k * n_tile])
                own_rows(n_down + 2 * k, n_down + 2 * k + 2)
        for b in range(uq_c // 128):
            cols = pl.ds(pl.multiple_of(h * uq_c + b * 128, 128), 128)
            wuq_t[b * 128:(b + 1) * 128, :] = wuq[:, cols].T
        for j in range(pairs):
            c0 = h * ukv_c + j * 2 * (nope + vdim)
            wa = wukv[:, pl.ds(pl.multiple_of(c0, 128), nope + vdim)]
            wb = wukv[:, pl.ds(pl.multiple_of(c0 + nope + vdim, 128), nope + vdim)]
            wk[:, 2 * nope * j:2 * nope * (j + 1)] = jnp.concatenate([wa[:, :nope], wb[:, :nope]], axis=1)
            wv_t[2 * vdim * j:2 * vdim * (j + 1), :] = jnp.concatenate([wa.T[nope:], wb.T[nope:]], axis=0)

        @pl.loop(0, n_tile)
        def _(t):
            it = h * n_tile + t
            for k in range(2 * n_tile):
                if k % n_tile and plan[first_iter + k]:
                    @pl.when(it == k)
                    def _(k=k):
                        pump(plan[first_iter + k])
            @pl.when(it >= 3)
            def _():
                o_copy(it - 3).wait()

            @pl.when(it >= 2)
            def _():
                o_copy(it - 2).start()

            slot = lax.rem(it, 2)
            rows = pl.ds(pl.multiple_of(t * TILE, TILE), TILE)
            cq = cq_t[:, rows]
            for g in range(half_heads // chunk):
                w = wuq_t[g * chunk * hd:(g + 1) * chunk * hd, :]
                q = jnp.dot(w, cq, preferred_element_type=F32)
                for hh in range(chunk):
                    j, side = (g * chunk + hh) // 2, hh % 2
                    r0 = hh * hd
                    for p in range(2):
                        lanes = slice(seq * p, seq * (p + 1))
                        dst = slice(seq * side, seq * (side + 1))
                        qs[p, j, side * nope:(side + 1) * nope, dst] = q[r0:r0 + nope, lanes].astype(BF16)
                        lo = q[r0 + nope:r0 + nope + hr, lanes]
                        hi = q[r0 + nope + hr:r0 + hd, lanes]
                        qs[p, j, 2 * nope:2 * nope + hr, dst] = (lo * cos_q - hi * sin_q).astype(BF16)
                        qs[p, j, 2 * nope + hr:2 * nope + rope, dst] = (hi * cos_q + lo * sin_q).astype(BF16)
            lat = c_s[rows, :]
            ks[...] = jnp.dot(lat, wk[...], preferred_element_type=F32).astype(BF16)
            v = jnp.dot(wv_t[...], c_t[:, rows], preferred_element_type=F32).astype(BF16)
            for j in range(pairs):
                vs[slot, j, :2 * vdim, :] = v[2 * vdim * j:2 * vdim * (j + 1)]

            r_blk = [r_s[pl.ds(pl.multiple_of(t * TILE + p * seq, seq), seq), :] for p in range(2)]
            def scores(p, j):
                lhs = jnp.concatenate([ks[seq * p:seq * (p + 1), 2 * nope * j:2 * nope * (j + 1)], r_blk[p]], axis=1)
                s = jnp.dot(lhs, qs[p, j], preferred_element_type=F32)
                s = jnp.where(diff_s[...] >= 0, s, fill)
                s_buf[p, j] = s
                k = p * pairs + j
                top = jnp.max(s.reshape(groups, 8, 2 * seq), axis=0)
                pm[8 * k:8 * (k + 1), :] = top[:, :seq]
                pm[16 * pairs + 8 * k:16 * pairs + 8 * (k + 1), :] = top[:, seq:]

            for j in range(pairs):
                scores(0, j)
                values(1, j, 1 - slot, lax.rem(it + 2, 3))
            maxima(0)

            for j in range(pairs):
                scores(1, j)
                values(0, j, slot, lax.rem(it, 3))
            maxima(1)

    last = 2 * n_tile - 1
    o_copy(last - 2).wait()
    o_copy(last - 1).start()
    for j in range(pairs):
        values(1, j, last % 2, last % 3)
    o_copy(last).start()

    pump(plan[first_iter + 2 * n_tile])
    stage_out.wait()
    o_copy(last - 1).wait()
    o_copy(last).wait()
    c_out.wait()
    r_out.wait()
    for step in range(1, n_dev):
        gain_copy(step).wait_send()
    for it in items:
        for t in range(N_MSG):
            send(it, t).wait_send()


def out_kernel(o_ref, w_ref, x_ref, c_ref, r_ref, y_ref, c_out, r_out):
    acc = jnp.dot(o_ref[...], w_ref[...], preferred_element_type=F32)
    y_ref[...] = (x_ref[...].astype(F32) + acc).astype(BF16)
    c_out[...] = c_ref[...]
    seq = r_out.shape[2]
    for p in range(r_out.shape[0]):
        r_out[p] = r_ref[p * seq:(p + 1) * seq, :].T[:r_out.shape[1]]


def solution(mesh):
    batch_spec = P(('dp', 'fsdp'))
    row_spec = P('fsdp')
    mat_spec = P('fsdp', None)
    n_dev = mesh.shape['fsdp']
    assert n_dev == 8 and mesh.shape['dp'] % 2 == 0

    def local_block(tok, g_in, w_dq, g_q, w_uq, w_dkv, g_kv, w_ukv, w_out):
        n_p, seq, d_model = tok.shape
        n_tok = n_p * seq
        kv_rank, q_rank = g_kv.shape[0] * n_dev, g_q.shape[0] * n_dev
        rope = w_dkv.shape[1] - kv_rank
        nope_total = w_ukv.shape[1] - w_out.shape[0] * n_dev
        n_heads = (w_uq.shape[1] - nope_total) // rope
        nope = nope_total // n_heads
        vdim = w_out.shape[0] * n_dev // n_heads
        pairs = n_heads // 4
        hh = n_heads // 2
        x2 = tok.reshape(n_tok, d_model)
        gains = jnp.concatenate([g_in, g_q, g_kv]).astype(F32)
        gains = jnp.pad(gains, (0, -gains.shape[0] % 128))[None]
        cos, sin = rope_tables(seq, rope)
        cos_t, sin_t = jnp.asarray(cos.T), jnp.asarray(sin.T)
        reps = TILE // seq
        cos_n = jnp.asarray(np.tile(np.concatenate([cos, cos], 1), (reps, 1)))
        sin_n = jnp.asarray(np.tile(np.concatenate([-sin, sin], 1), (reps, 1)))
        dims = (n_dev, n_heads, nope, rope, vdim, d_model, q_rank, kv_rank, seq)
        n_items = len(SPLITS)
        any_ = pl.BlockSpec(memory_space=pl.ANY)
        vm = pl.BlockSpec(memory_space=pltpu.VMEM)
        o, wo_full, c_all, r_all = pl.pallas_call(
            functools.partial(gather_kernel, dims),
            out_shape=(
                jax.ShapeDtypeStruct((n_tok, n_heads * vdim), BF16),
                jax.ShapeDtypeStruct((n_heads * vdim, d_model), BF16),
                jax.ShapeDtypeStruct((n_tok, kv_rank), BF16),
                jax.ShapeDtypeStruct((n_tok, 128), BF16),
            ),
            in_specs=[any_] * 7 + [vm] * 4,
            out_specs=(any_,) * 4,
            scratch_shapes=[
                pltpu.VMEM((n_dev, 1, gains.shape[1]), F32),
                pltpu.VMEM((n_tok, d_model), BF16),
                pltpu.VMEM((d_model, q_rank), BF16),
                pltpu.VMEM((d_model, kv_rank + rope), BF16),
                pltpu.VMEM((n_tok, q_rank), F32),
                pltpu.VMEM((n_tok, kv_rank + rope), F32),
                pltpu.VMEM((q_rank, w_uq.shape[1]), BF16),
                pltpu.VMEM((w_uq.shape[1] // 2, q_rank), BF16),
                pltpu.VMEM((kv_rank, w_ukv.shape[1]), BF16),
                pltpu.VMEM((kv_rank, hh * nope), BF16),
                pltpu.VMEM((hh * vdim, kv_rank), BF16),
                pltpu.VMEM((q_rank, n_tok), BF16),
                pltpu.VMEM((n_tok, kv_rank), BF16),
                pltpu.VMEM((kv_rank, n_tok), BF16),
                pltpu.VMEM((n_tok, 128), BF16),
                pltpu.VMEM((2, pairs, 2 * nope + 128, 2 * seq), BF16),
                pltpu.VMEM((TILE, hh * nope), BF16),
                pltpu.VMEM((2, pairs, 2 * vdim + 16, TILE), BF16),
                pltpu.VMEM((3, TILE, hh * vdim), BF16),
                pltpu.VMEM(w_out.shape, BF16),
                pltpu.VMEM((seq, 2 * seq), jnp.int32),
                pltpu.VMEM((n_tok, 1), F32),
                pltpu.VMEM((8, d_model), F32),
                pltpu.VMEM((2, pairs, seq, 2 * seq), F32),
                pltpu.VMEM((2 * 2 * pairs * 8, seq), F32),
                pltpu.VMEM((2 * pairs, 2 * seq), F32),
                pltpu.SemaphoreType.DMA((n_items * N_MSG,)),
                pltpu.SemaphoreType.DMA((n_items * N_MSG,)),
                pltpu.SemaphoreType.DMA((10,)),
                pltpu.SemaphoreType.DMA((n_dev - 1,)),
                pltpu.SemaphoreType.DMA((n_dev - 1,)),
                pltpu.SemaphoreType.DMA((n_tok // TILE,)),
                pltpu.SemaphoreType.DMA((3,)),
                pltpu.SemaphoreType.DMA((2,)),
            ],
            compiler_params=pltpu.CompilerParams(
                collective_id=0, has_side_effects=True, vmem_limit_bytes=67_043_328
            ),
            name='gather_attend',
        )(x2, gains, w_dq, w_dkv, w_uq, w_ukv, w_out, cos_t, sin_t, cos_n, sin_n)

        bm, bn = 512, 1280
        n_m, n_n = n_tok // bm, d_model // bn
        once = lambda n, m: (jnp.where(n == 0, m, n_m - 1), 0)
        y, c_blk, r_blk = pl.pallas_call(
            out_kernel,
            grid=(n_n, n_m),
            in_specs=[
                pl.BlockSpec((bm, n_heads * vdim), lambda n, m: (m, 0)),
                pl.BlockSpec((n_heads * vdim, bn), lambda n, m: (0, n)),
                pl.BlockSpec((bm, bn), lambda n, m: (m, n)),
                pl.BlockSpec((bm, kv_rank), once),
                pl.BlockSpec((bm, 128), once),
            ],
            out_specs=[
                pl.BlockSpec((bm, bn), lambda n, m: (m, n)),
                pl.BlockSpec((bm, kv_rank), once),
                pl.BlockSpec((bm // seq, rope, seq), lambda n, m: (jnp.where(n == 0, m, n_m - 1), 0, 0)),
            ],
            out_shape=[
                jax.ShapeDtypeStruct((n_tok, d_model), BF16),
                jax.ShapeDtypeStruct((n_tok, kv_rank), BF16),
                jax.ShapeDtypeStruct((n_p, rope, seq), BF16),
            ],
            compiler_params=pltpu.CompilerParams(vmem_limit_bytes=60 * 1024 * 1024),
            name='project_out',
        )(o, wo_full, x2, c_all, r_all)
        return y.reshape(tok.shape), c_blk.reshape(n_p, seq, kv_rank), jnp.swapaxes(r_blk, 1, 2)

    return jax.shard_map(
        local_block,
        mesh=mesh,
        in_specs=(batch_spec, row_spec, mat_spec, row_spec, mat_spec, mat_spec, row_spec, mat_spec, mat_spec),
        out_specs=(batch_spec, batch_spec, batch_spec),
        check_vma=False,
    )
```

```python
import functools

import jax
import jax.numpy as jnp
import numpy as np
from jax import lax
from jax.experimental import pallas as pl
from jax.experimental.pallas import tpu as pltpu
from jax.sharding import PartitionSpec as P

EPSILON = 1e-6
ROPE_THETA = 10000.0
MESH = pl.DeviceIdType.MESH
BF16 = jnp.bfloat16
F32 = jnp.float32
N_MSG = 14
TILE = 256
NORM = 128


def rope_tables(seq_len, rope_dim):
    half_dim = rope_dim // 2
    expo = (-2.0 * np.arange(half_dim, dtype=np.float32) / np.float32(rope_dim)).astype(np.float32)
    inv_freq = np.power(np.float32(ROPE_THETA), expo).astype(np.float32)
    angles = np.arange(seq_len, dtype=np.float32)[:, None] * inv_freq[None, :]
    return np.cos(angles).astype(np.float32), np.sin(angles).astype(np.float32)


def rms(v, gain):
    return v * lax.rsqrt(jnp.mean(v * v, axis=-1, keepdims=True) + EPSILON) * gain


THEN = {0: (3, 5, 8), 1: (4, 6, 9), 3: (7,), 4: (10,), 5: (11,), 6: (12,), 7: (13,)}
ROUTE = 'RLDRLZZZDDDDDD'
SPLITS = ((112, 112), (80, 128), (96, 96), (32, 32), (640, 640), (32, 32), (896, 896),
          (112, 160), (112, 112), (64, 80), (64, 64))
T_NORM, T_DOWN, T_PREP, T_ITER = 1.7, 5.2, 1.9, 2.7


def plan_transfers(pieces, steps, first):
    rate = {'R': 42e3, 'L': 42e3, 'Z': 42e3, 'D': 200e3}
    hop = {'R': 3.0, 'L': 3.0, 'Z': 3.0, 'D': 2.0}
    free = dict.fromkeys(rate, 0.0)
    state = {'now': 2.5, 'next': 0}
    arrival, done, lists = {}, set(), []

    def send(i, t):
        n, p, r, unit = pieces[i]
        pm = n - p
        size = (pm, pm, n, r, pm - r, p, p, p, pm, pm, pm, p, p, p)[t] * unit
        link = ROUTE[t]
        free[link] = max(state['now'], free[link]) + size / rate[link]
        arrival[i, t] = free[link] + hop[link]

    def own(out):
        i = state['next']
        state['next'] = i + 1
        for t in (0, 1, 2):
            send(i, t)
        out.append((i, -1))

    def wait(i, t, out):
        state['now'] = max(state['now'], arrival[i, t])
        done.add((i, t))
        out.append((i, t))
        for u in THEN.get(t, ()):
            send(i, u)

    for k, (need, busy) in enumerate(steps):
        out = []
        while True:
            while state['next'] < len(pieces) and (
                k == 0 and state['next'] < first or min(free['R'], free['L']) - state['now'] < 2
                and all((i, t) in done for i in range(first) for t in (0, 1))
            ):
                own(out)
            ready = sorted(
                (a, i, t) for (i, t), a in arrival.items()
                if (i, t) not in done and t in THEN and (t != 4 or (i, 3) in done)
            )
            if ready and ready[0][0] + 0.3 <= state['now']:
                wait(*ready[0][1:], out)
                continue
            missing = [m for m in need if m not in done]
            if not missing:
                break
            here = [m for m in missing if m in arrival and arrival[m] <= state['now']]
            if here:
                wait(*here[0], out)
                continue
            ready += [(arrival[m], *m) for m in missing if m in arrival and m[1] not in THEN]
            wait(*min(ready)[1:], out)
        lists.append(out)
        state['now'] += busy
    return lists


class Item:
    def __init__(self, index, local, full, rows, by_rows, split, col0, cols):
        self.index, self.local, self.full = index, local, full
        self.rows, self.by_rows = rows, by_rows
        self.s, self.h = split
        self.col0, self.cols = col0, cols
        self.span = rows if by_rows else cols

    def _cut(self, ref, row0, off, size):
        if self.by_rows:
            rows = pl.ds(pl.multiple_of(row0 + off, 16), size)
            cols = pl.ds(self.col0, self.cols)
        else:
            rows = pl.ds(row0 if isinstance(row0, int) else pl.multiple_of(row0, 16), self.rows)
            cols = pl.ds(pl.multiple_of(self.col0 + off, 128), size)
        return ref.at[rows, cols]

    def mine(self, off, size):
        return self._cut(self.local, 0, off, size)

    def at(self, origin, off, size):
        return self._cut(self.full, origin * self.rows, off, size)


def gather_kernel(
    dims, x_hbm, gains_hbm, wdq_l, wdkv_l, wuq_l, wukv_l, wo_l, cos_t, sin_t, cos_n, sin_n,
    o_hbm, wo_full, c_hbm, r_hbm,
    gbuf, a_s, wdq, wdkv, wdkv_t, acc_q, acc_kv, wuq, wuq_t, wukv, wk, wv_t,
    cq_t, c_s, c_t, r_s, qs, ks, vs, o_s, stage, diff_s, inv_s, gb_s, s_buf, pm, ms,
    ssem, rsem, lsem, gssem, grsem, xsem, osem, csem,
):
    n_dev, n_heads, nope, rope, vdim, d_model, q_rank, kv_rank, seq = dims
    f = lax.axis_index('fsdp')
    d = lax.axis_index('dp')
    core = lax.rem(f, 2)
    par = lax.rem(d, 2)
    chip = f // 2
    n_chip = n_dev // 2
    mod = lambda v: lax.rem(v, n_dev)
    right, left, opp = mod(f + 2), mod(f + n_dev - 2), mod(f + 4)
    partner = f + 1 - 2 * core
    p_right, p_left, p_opp = mod(partner + 2), mod(partner + n_dev - 2), mod(partner + 4)
    d_pair = d + 1 - 2 * par
    to_right, to_left, to_partner, to_pair = (d, right), (d, left), (d, partner), (d_pair, f)
    n_tok = a_s.shape[0]
    n_tile = n_tok // TILE
    half_heads = n_heads // 2
    pairs = half_heads // 2
    hd = nope + rope

    barrier = pltpu.get_barrier_semaphore()
    for step in range(1, n_dev):
        pl.semaphore_signal(barrier, inc=1, device_id=(d, mod(f + step)), device_id_type=MESH)
    pl.semaphore_signal(barrier, inc=1, device_id=to_pair, device_id_type=MESH)
    x_in = [
        pltpu.make_async_copy(x_hbm.at[pl.ds(TILE * t, TILE)], a_s.at[pl.ds(TILE * t, TILE)], xsem.at[t])
        for t in range(n_tile)
    ]
    for cp in x_in:
        cp.start()
    gain_in = pltpu.make_async_copy(gains_hbm, gbuf.at[f], lsem.at[9])
    gain_in.start()
    pl.semaphore_wait(barrier, n_dev)

    r_d, r_q, r_kv, r_o = wdq_l.shape[0], wuq_l.shape[0], wukv_l.shape[0], wo_l.shape[0]
    n_d, n_o = 2, 4
    dq_c, uq_c, ukv_c, o_c = wdq_l.shape[1] // n_d, wuq_l.shape[1] // 2, wukv_l.shape[1] // 2, wo_l.shape[1] // n_o
    parts = [(wdq_l, wdq, r_d, True, h * dq_c, dq_c) for h in range(n_d)]
    r_dkv = wdkv_l.shape[0]
    parts.append((wdkv_l, wdkv_t, r_dkv, True, 0, wdkv_l.shape[1]))
    n_down = len(parts)
    for h in range(2):
        parts.append((wuq_l, wuq, r_q, True, h * uq_c, uq_c))
        parts.append((wukv_l, wukv, r_kv, False, h * ukv_c, ukv_c))
    n_head = len(parts)
    parts += [(wo_l, wo_full, r_o, True, h * o_c, o_c) for h in range(n_o)]
    items = [Item(k, *p[:4], SPLITS[k], *p[4:]) for k, p in enumerate(parts)]

    everything = range(N_MSG)
    needs = lambda lo, hi, ts=everything: [(i, t) for i in range(lo, hi) for t in ts]
    n_pre = 7
    steps = [([], T_NORM)] * n_pre
    stages = []
    for need, cost, every in (
        (needs(0, n_down, (2,)), T_DOWN, 2),
        (needs(0, n_down, (0, 1, 5, 6, 8, 9, 11, 12)), 2 * T_DOWN, 1),
        (needs(0, n_down), 1.2 * T_DOWN, 1),
    ):
        stages.append((len(steps) + 1, every))
        steps += [(need if t == 0 else [], cost * every / n_tile) for t in range(0, n_tile, every)]
    first_iter = len(steps) + 1
    for h in range(2):
        for t in range(n_tile):
            need = needs(n_down + 2 * h, n_down + 2 * h + 2) if t == 0 else []
            steps.append((need, T_ITER + (T_PREP if t == 0 else 0)))
    steps.append((needs(n_head, len(parts)), 0))
    pieces = [
        (it.span, it.s, it.h, 2 * (-(-it.cols // 128) * 128 if it.by_rows else it.rows)) for it in items
    ]
    plan = plan_transfers(pieces, [([], 0)] + steps, n_down)

    def messages(it):
        n, s, h = it.span, it.s, it.h
        own_p, pm_off, other_p = par * (n - s), par * s, (1 - par) * (n - s)
        pm, m = n - s, n - s - h
        h_off, m_off = par * (n - h), (1 - par) * h + par * s
        reg = it.at
        return [
            (it.mine(pm_off, pm), reg(f, pm_off, pm), to_right, reg(left, pm_off, pm)),
            (it.mine(pm_off, pm), reg(f, pm_off, pm), to_left, reg(right, pm_off, pm)),
            (it.mine(0, n), reg(f, 0, n), to_partner, reg(partner, 0, n)),
            (reg(left, h_off, h), reg(left, h_off, h), to_right, reg(opp, h_off, h)),
            (reg(right, m_off, m), reg(right, m_off, m), to_left, reg(opp, m_off, m)),
            (reg(left, own_p, s), reg(left, own_p, s), to_pair, reg(left, other_p, s)),
            (reg(right, own_p, s), reg(right, own_p, s), to_pair, reg(right, other_p, s)),
            (reg(opp, own_p, s), reg(opp, own_p, s), to_pair, reg(opp, other_p, s)),
            (reg(left, pm_off, pm), reg(left, pm_off, pm), to_partner, reg(p_left, pm_off, pm)),
            (reg(right, pm_off, pm), reg(right, pm_off, pm), to_partner, reg(p_right, pm_off, pm)),
            (reg(opp, pm_off, pm), reg(opp, pm_off, pm), to_partner, reg(p_opp, pm_off, pm)),
            (reg(left, other_p, s), reg(left, other_p, s), to_partner, reg(p_left, other_p, s)),
            (reg(right, other_p, s), reg(right, other_p, s), to_partner, reg(p_right, other_p, s)),
            (reg(opp, other_p, s), reg(opp, other_p, s), to_partner, reg(p_opp, other_p, s)),
        ]

    def send(it, t):
        src, dst, dev, _ = messages(it)[t]
        k = it.index * N_MSG + t
        return pltpu.make_async_remote_copy(src, dst, ssem.at[k], rsem.at[k], device_id=dev, device_id_type=MESH)

    def recv(it, t):
        _, _, dev, got = messages(it)[t]
        k = it.index * N_MSG + t
        return pltpu.make_async_remote_copy(got, got, ssem.at[k], rsem.at[k], device_id=dev, device_id_type=MESH)

    def start(it, *ts):
        for t in ts:
            send(it, t).start()

    def got(it, *ts):
        for t in ts:
            recv(it, t).wait_recv()

    def local_copy(it):
        return pltpu.make_async_copy(it.mine(0, it.span), it.at(f, 0, it.span), lsem.at[it.index])

    stage_in = pltpu.make_async_copy(wo_l, stage, lsem.at[n_head])
    stage_out = pltpu.make_async_copy(stage, wo_full.at[pl.ds(pl.multiple_of(f * r_o, 16), r_o)], lsem.at[n_head + 1])

    def pump(segment):
        for i, t in segment:
            it = items[i]
            if t < 0:
                start(it, 0, 1, 2)
                if i < n_head:
                    local_copy(it).start()
            else:
                got(it, t)
                start(it, *THEN.get(t, ()))

    def own_rows(first, last):
        for i in range(first, last):
            local_copy(items[i]).wait()

    def gain_copy(step):
        return pltpu.make_async_remote_copy(
            gbuf.at[f], gbuf.at[f], gssem.at[step - 1], grsem.at[step - 1],
            device_id=(d, mod(f + step)), device_id_type=MESH,
        )

    gain_in.wait()
    for step in range(1, n_dev):
        gain_copy(step).start()
    pump(plan[0])
    stage_in.start()

    row_i = lax.broadcasted_iota(jnp.int32, (seq, 2 * seq), 0)
    lane_i = lax.broadcasted_iota(jnp.int32, (seq, 2 * seq), 1)
    diff_s[...] = lax.rem(lane_i, seq) - row_i
    for p in range(2):
        @pl.loop(0, pairs)
        def _(j, p=p):
            qs[p, j] = jnp.zeros(qs.shape[2:], BF16)

    @pl.loop(0, pairs)
    def _(j):
        for b in range(2):
            vs[b, j, :2 * vdim, :] = jnp.zeros((2 * vdim, vs.shape[3]), BF16)
            vs[b, j, 2 * vdim:, :] = jnp.ones((vs.shape[2] - 2 * vdim, vs.shape[3]), BF16)
        s_buf[1, j] = jnp.zeros(s_buf.shape[2:], F32)

    r_s[...] = jnp.zeros(r_s.shape, BF16)
    ms[...] = jnp.zeros(ms.shape, F32)

    for t, cp in enumerate(x_in):
        if t in (n_tile // 2, 3 * n_tile // 4):
            pump(plan[1 if t == n_tile // 2 else 2])
        cp.wait()
        v = a_s[TILE * t:TILE * (t + 1), :].astype(F32)
        inv_s[TILE * t:TILE * (t + 1), :] = lax.rsqrt(jnp.mean(v * v, axis=-1, keepdims=True) + EPSILON)

    for step in range(1, n_dev):
        gain_copy(step).wait_recv()
    n_in, n_q, n_kv = d_model // n_dev, q_rank // n_dev, kv_rank // n_dev
    join = lambda lo, n: jnp.concatenate([gbuf[i][:, lo:lo + n] for i in range(n_dev)], axis=1)
    g_in, g_q, g_kv = join(0, n_in), join(n_in, n_q), join(n_in + n_q, n_kv)

    gb_s[...] = jnp.broadcast_to(g_in, gb_s.shape)
    pump(plan[3])
    n_norm = n_tok // NORM

    @pl.loop(0, n_norm)
    def _(t):
        for k in range(1, 4):
            @pl.when(t == k * n_norm // 4)
            def _(k=k):
                pump(plan[3 + k])
        rows = pl.ds(pl.multiple_of(t * NORM, NORM), NORM)
        v = a_s[rows, :].astype(F32) * inv_s[rows, :]
        v = v.reshape(NORM // 8, 8, d_model) * gb_s[...][None]
        a_s[rows, :] = v.reshape(NORM, d_model).astype(BF16)

    pump(plan[n_pre])

    depth = 2 * r_d

    chip_cols = lambda c: pl.ds(pl.multiple_of(lax.rem(chip + c, n_chip) * depth, 128), depth)
    tile_rows = lambda t: pl.ds(pl.multiple_of(t * TILE, TILE), TILE)

    def down(t, hops):
        rows = tile_rows(t)
        cols = [chip_cols(c) for c in hops]
        a = jnp.concatenate([a_s[rows, c] for c in cols], axis=1)
        for w, acc in ((wdq, acc_q), (wdkv, acc_kv)):
            part = jnp.dot(a, jnp.concatenate([w[c, :] for c in cols], axis=0), preferred_element_type=F32)
            if hops[0] == 0:
                acc[rows, :] = part
            else:
                acc[rows, :] += part

    def turn(hops):
        for c in hops:
            for k in range(2):
                origin = lax.rem(chip + c, n_chip) * 2 + k
                block = wdkv_t[pl.ds(pl.multiple_of(origin * r_dkv, 16), r_dkv), :]
                wdkv[pl.ds(pl.multiple_of(origin * r_d, 16), r_d), :] = block.T

    def finish(t):
        rows = tile_rows(t)
        cq_t[:, rows] = rms(acc_q[rows, :], g_q).astype(BF16).T
        kv = acc_kv[rows, :]
        lat = rms(kv[:, :kv_rank], g_kv).astype(BF16)
        c_s[rows, :] = lat
        c_t[:, rows] = lat.T
        pe = kv[:, kv_rank:]
        swapped = jnp.concatenate([pe[:, rope // 2:], pe[:, :rope // 2]], axis=1)
        r_s[rows, :rope] = (pe * cos_n[...] + swapped * sin_n[...]).astype(BF16)

    own_rows(0, n_down)
    def look(stage, t):
        base, every = stages[stage]
        for q in range(1, n_tile // every):
            if plan[base + q]:
                @pl.when(t == q * every)
                def _(q=q):
                    pump(plan[base + q])

    for k, hops in enumerate(((0,), (n_chip - 1, 1))):
        pump(plan[stages[k][0]])
        turn(hops)

        @pl.loop(0, n_tile)
        def _(t):
            look(k, t)
            down(t, hops)

    pump(plan[stages[2][0]])
    turn((2,))
    down(0, (2,))

    @pl.loop(1, n_tile)
    def _(t):
        look(2, t)
        down(t, (2,))
        finish(t - 1)

    finish(n_tile - 1)
    stage_in.wait()
    stage_out.start()
    c_out = pltpu.make_async_copy(c_s, c_hbm, csem.at[0])
    r_out = pltpu.make_async_copy(r_s, r_hbm, csem.at[1])
    c_out.start()
    r_out.start()

    scale = float((nope + rope) ** -0.5)
    exp_scale = scale * float(np.log2(np.e))
    fill = -1e30 / scale
    cos_q, sin_q = cos_t[...], sin_t[...]
    hr = rope // 2

    def o_copy(it):
        h, t, slot = it // n_tile, it % n_tile, it % 3
        return pltpu.make_async_copy(
            o_s.at[slot],
            o_hbm.at[pl.ds(pl.multiple_of(t * TILE, TILE), TILE),
                     pl.ds(pl.multiple_of(h * half_heads * vdim, 128), half_heads * vdim)],
            osem.at[slot],
        )

    groups = seq // 8

    def maxima(p):
        for side in range(2):
            base = 16 * pairs * side + 8 * pairs * p
            part = [pm[pl.ds(base + i, pairs, stride=8), :] for i in range(8)]
            ms[pairs * p:pairs * (p + 1), seq * side:seq * (side + 1)] = functools.reduce(jnp.maximum, part)

    def values(p, j, slot, o_slot):
        k = p * pairs + j
        m = jnp.broadcast_to(ms[k:k + 1, :], (8, 2 * seq))
        s = s_buf[p, j].reshape(groups, 8, 2 * seq)
        e = jnp.exp2((s - m[None]) * exp_scale).astype(BF16).reshape(seq, 2 * seq)
        ov = jnp.dot(vs[slot, j, :, seq * p:seq * (p + 1)], e, preferred_element_type=F32)
        inv = (1.0 / ov[2 * vdim:2 * vdim + 8, :])[None]
        oa = ov[:vdim, :seq].reshape(vdim // 8, 8, seq) * inv[:, :, :seq]
        ob = ov[vdim:2 * vdim, seq:].reshape(vdim // 8, 8, seq) * inv[:, :, seq:]
        o_t = jnp.concatenate([oa, ob], axis=0).reshape(2 * vdim, seq).astype(BF16)
        o_s[o_slot, seq * p:seq * (p + 1), 2 * vdim * j:2 * vdim * (j + 1)] = o_t.T

    chunk = 4

    @pl.loop(0, 2)
    def _(h):
        for k in range(2):
            @pl.when(h == k)
            def _(k=k):
                pump(plan[first_iter + k * n_tile])
                own_rows(n_down + 2 * k, n_down + 2 * k + 2)
        for b in range(uq_c // 128):
            cols = pl.ds(pl.multiple_of(h * uq_c + b * 128, 128), 128)
            wuq_t[b * 128:(b + 1) * 128, :] = wuq[:, cols].T
        for j in range(pairs):
            c0 = h * ukv_c + j * 2 * (nope + vdim)
            wa = wukv[:, pl.ds(pl.multiple_of(c0, 128), nope + vdim)]
            wb = wukv[:, pl.ds(pl.multiple_of(c0 + nope + vdim, 128), nope + vdim)]
            wk[:, 2 * nope * j:2 * nope * (j + 1)] = jnp.concatenate([wa[:, :nope], wb[:, :nope]], axis=1)
            wv_t[2 * vdim * j:2 * vdim * (j + 1), :] = jnp.concatenate([wa.T[nope:], wb.T[nope:]], axis=0)

        @pl.loop(0, n_tile)
        def _(t):
            it = h * n_tile + t
            for q in range(4):
                @pl.when(it // (n_tile // 2) == q)
                def _(q=q):
                    for k in range(q * n_tile // 2, (q + 1) * n_tile // 2):
                        if k % n_tile and plan[first_iter + k]:
                            @pl.when(it == k)
                            def _(k=k):
                                pump(plan[first_iter + k])

            @pl.when(it >= 3)
            def _():
                o_copy(it - 3).wait()

            @pl.when(it >= 2)
            def _():
                o_copy(it - 2).start()

            slot = lax.rem(it, 2)
            rows = pl.ds(pl.multiple_of(t * TILE, TILE), TILE)
            cq = cq_t[:, rows]
            for g in range(half_heads // chunk):
                w = wuq_t[g * chunk * hd:(g + 1) * chunk * hd, :]
                q = jnp.dot(w, cq, preferred_element_type=F32)
                for hh in range(chunk):
                    j, side = (g * chunk + hh) // 2, hh % 2
                    r0 = hh * hd
                    for p in range(2):
                        lanes = slice(seq * p, seq * (p + 1))
                        dst = slice(seq * side, seq * (side + 1))
                        qs[p, j, side * nope:(side + 1) * nope, dst] = q[r0:r0 + nope, lanes].astype(BF16)
                        lo = q[r0 + nope:r0 + nope + hr, lanes]
                        hi = q[r0 + nope + hr:r0 + hd, lanes]
                        qs[p, j, 2 * nope:2 * nope + hr, dst] = (lo * cos_q - hi * sin_q).astype(BF16)
                        qs[p, j, 2 * nope + hr:2 * nope + rope, dst] = (hi * cos_q + lo * sin_q).astype(BF16)
            lat = c_s[rows, :]
            ks[...] = jnp.dot(lat, wk[...], preferred_element_type=F32).astype(BF16)
            v = jnp.dot(wv_t[...], c_t[:, rows], preferred_element_type=F32).astype(BF16)
            for j in range(pairs):
                vs[slot, j, :2 * vdim, :] = v[2 * vdim * j:2 * vdim * (j + 1)]

            r_blk = [r_s[pl.ds(pl.multiple_of(t * TILE + p * seq, seq), seq), :] for p in range(2)]
            def scores(p, j):
                lhs = jnp.concatenate([ks[seq * p:seq * (p + 1), 2 * nope * j:2 * nope * (j + 1)], r_blk[p]], axis=1)
                s = jnp.dot(lhs, qs[p, j], preferred_element_type=F32)
                s = jnp.where(diff_s[...] >= 0, s, fill)
                s_buf[p, j] = s
                k = p * pairs + j
                top = jnp.max(s.reshape(groups, 8, 2 * seq), axis=0)
                pm[8 * k:8 * (k + 1), :] = top[:, :seq]
                pm[16 * pairs + 8 * k:16 * pairs + 8 * (k + 1), :] = top[:, seq:]

            for j in range(pairs):
                scores(0, j)
                values(1, j, 1 - slot, lax.rem(it + 2, 3))
            maxima(0)

            for j in range(pairs):
                scores(1, j)
                values(0, j, slot, lax.rem(it, 3))
            maxima(1)

    last = 2 * n_tile - 1
    o_copy(last - 2).wait()
    o_copy(last - 1).start()
    for j in range(pairs):
        values(1, j, last % 2, last % 3)
    o_copy(last).start()

    pump(plan[first_iter + 2 * n_tile])
    stage_out.wait()
    o_copy(last - 1).wait()
    o_copy(last).wait()
    c_out.wait()
    r_out.wait()
    for step in range(1, n_dev):
        gain_copy(step).wait_send()
    for it in items:
        for t in range(N_MSG):
            send(it, t).wait_send()


def out_kernel(o_ref, w_ref, x_ref, c_ref, r_ref, y_ref, c_out, r_out):
    acc = jnp.dot(o_ref[...], w_ref[...], preferred_element_type=F32)
    y_ref[...] = (x_ref[...].astype(F32) + acc).astype(BF16)
    c_out[...] = c_ref[...]
    seq = r_out.shape[2]
    for p in range(r_out.shape[0]):
        r_out[p] = r_ref[p * seq:(p + 1) * seq, :].T[:r_out.shape[1]]


def solution(mesh):
    batch_spec = P(('dp', 'fsdp'))
    row_spec = P('fsdp')
    mat_spec = P('fsdp', None)
    n_dev = mesh.shape['fsdp']
    assert n_dev == 8 and mesh.shape['dp'] % 2 == 0

    def local_block(tok, g_in, w_dq, g_q, w_uq, w_dkv, g_kv, w_ukv, w_out):
        n_p, seq, d_model = tok.shape
        n_tok = n_p * seq
        kv_rank, q_rank = g_kv.shape[0] * n_dev, g_q.shape[0] * n_dev
        rope = w_dkv.shape[1] - kv_rank
        nope_total = w_ukv.shape[1] - w_out.shape[0] * n_dev
        n_heads = (w_uq.shape[1] - nope_total) // rope
        nope = nope_total // n_heads
        vdim = w_out.shape[0] * n_dev // n_heads
        pairs = n_heads // 4
        hh = n_heads // 2
        x2 = tok.reshape(n_tok, d_model)
        gains = jnp.concatenate([g_in, g_q, g_kv]).astype(F32)
        gains = jnp.pad(gains, (0, -gains.shape[0] % 128))[None]
        cos, sin = rope_tables(seq, rope)
        cos_t, sin_t = jnp.asarray(cos.T), jnp.asarray(sin.T)
        reps = TILE // seq
        cos_n = jnp.asarray(np.tile(np.concatenate([cos, cos], 1), (reps, 1)))
        sin_n = jnp.asarray(np.tile(np.concatenate([-sin, sin], 1), (reps, 1)))
        dims = (n_dev, n_heads, nope, rope, vdim, d_model, q_rank, kv_rank, seq)
        n_items = len(SPLITS)
        any_ = pl.BlockSpec(memory_space=pl.ANY)
        vm = pl.BlockSpec(memory_space=pltpu.VMEM)
        o, wo_full, c_all, r_all = pl.pallas_call(
            functools.partial(gather_kernel, dims),
            out_shape=(
                jax.ShapeDtypeStruct((n_tok, n_heads * vdim), BF16),
                jax.ShapeDtypeStruct((n_heads * vdim, d_model), BF16),
                jax.ShapeDtypeStruct((n_tok, kv_rank), BF16),
                jax.ShapeDtypeStruct((n_tok, 128), BF16),
            ),
            in_specs=[any_] * 7 + [vm] * 4,
            out_specs=(any_,) * 4,
            scratch_shapes=[
                pltpu.VMEM((n_dev, 1, gains.shape[1]), F32),
                pltpu.VMEM((n_tok, d_model), BF16),
                pltpu.VMEM((d_model, q_rank), BF16),
                pltpu.VMEM((d_model, kv_rank + rope), BF16),
                pltpu.VMEM((n_dev * w_dkv.shape[1], w_dkv.shape[0]), BF16),
                pltpu.VMEM((n_tok, q_rank), F32),
                pltpu.VMEM((n_tok, kv_rank + rope), F32),
                pltpu.VMEM((q_rank, w_uq.shape[1]), BF16),
                pltpu.VMEM((w_uq.shape[1] // 2, q_rank), BF16),
                pltpu.VMEM((kv_rank, w_ukv.shape[1]), BF16),
                pltpu.VMEM((kv_rank, hh * nope), BF16),
                pltpu.VMEM((hh * vdim, kv_rank), BF16),
                pltpu.VMEM((q_rank, n_tok), BF16),
                pltpu.VMEM((n_tok, kv_rank), BF16),
                pltpu.VMEM((kv_rank, n_tok), BF16),
                pltpu.VMEM((n_tok, 128), BF16),
                pltpu.VMEM((2, pairs, 2 * nope + 128, 2 * seq), BF16),
                pltpu.VMEM((TILE, hh * nope), BF16),
                pltpu.VMEM((2, pairs, 2 * vdim + 16, TILE), BF16),
                pltpu.VMEM((3, TILE, hh * vdim), BF16),
                pltpu.VMEM(w_out.shape, BF16),
                pltpu.VMEM((seq, 2 * seq), jnp.int32),
                pltpu.VMEM((n_tok, 1), F32),
                pltpu.VMEM((8, d_model), F32),
                pltpu.VMEM((2, pairs, seq, 2 * seq), F32),
                pltpu.VMEM((2 * 2 * pairs * 8, seq), F32),
                pltpu.VMEM((2 * pairs, 2 * seq), F32),
                pltpu.SemaphoreType.DMA((n_items * N_MSG,)),
                pltpu.SemaphoreType.DMA((n_items * N_MSG,)),
                pltpu.SemaphoreType.DMA((10,)),
                pltpu.SemaphoreType.DMA((n_dev - 1,)),
                pltpu.SemaphoreType.DMA((n_dev - 1,)),
                pltpu.SemaphoreType.DMA((n_tok // TILE,)),
                pltpu.SemaphoreType.DMA((3,)),
                pltpu.SemaphoreType.DMA((2,)),
            ],
            compiler_params=pltpu.CompilerParams(
                collective_id=0, has_side_effects=True, vmem_limit_bytes=67_043_328,
            ),
            name='gather_attend',
        )(x2, gains, w_dq, w_dkv.T, w_uq, w_ukv, w_out, cos_t, sin_t, cos_n, sin_n)

        bm, bn = 512, 1280
        n_m, n_n = n_tok // bm, d_model // bn
        once = lambda n, m: (jnp.where(n == 0, m, n_m - 1), 0)
        y, c_blk, r_blk = pl.pallas_call(
            out_kernel,
            grid=(n_n, n_m),
            in_specs=[
                pl.BlockSpec((bm, n_heads * vdim), lambda n, m: (m, 0)),
                pl.BlockSpec((n_heads * vdim, bn), lambda n, m: (0, n)),
                pl.BlockSpec((bm, bn), lambda n, m: (m, n)),
                pl.BlockSpec((bm, kv_rank), once),
                pl.BlockSpec((bm, 128), once),
            ],
            out_specs=[
                pl.BlockSpec((bm, bn), lambda n, m: (m, n)),
                pl.BlockSpec((bm, kv_rank), once),
                pl.BlockSpec((bm // seq, rope, seq), lambda n, m: (jnp.where(n == 0, m, n_m - 1), 0, 0)),
            ],
            out_shape=[
                jax.ShapeDtypeStruct((n_tok, d_model), BF16),
                jax.ShapeDtypeStruct((n_tok, kv_rank), BF16),
                jax.ShapeDtypeStruct((n_p, rope, seq), BF16),
            ],
            compiler_params=pltpu.CompilerParams(vmem_limit_bytes=60 * 1024 * 1024),
            name='project_out',
        )(o, wo_full, x2, c_all, r_all)
        return y.reshape(tok.shape), c_blk.reshape(n_p, seq, kv_rank), jnp.swapaxes(r_blk, 1, 2)

    return jax.shard_map(
        local_block,
        mesh=mesh,
        in_specs=(batch_spec, row_spec, mat_spec, row_spec, mat_spec, mat_spec, row_spec, mat_spec, mat_spec),
        out_specs=(batch_spec, batch_spec, batch_spec),
        check_vma=False,
    )
```

```python
import functools

import jax
import jax.numpy as jnp
import numpy as np
from jax import lax
from jax.experimental import pallas as pl
from jax.experimental.pallas import tpu as pltpu
from jax.sharding import PartitionSpec as P

EPSILON = 1e-6
ROPE_THETA = 10000.0
MESH = pl.DeviceIdType.MESH
BF16 = jnp.bfloat16
F32 = jnp.float32
N_MSG = 14
TILE = 256
NORM = 128


def rope_tables(seq_len, rope_dim):
    half_dim = rope_dim // 2
    expo = (-2.0 * np.arange(half_dim, dtype=np.float32) / np.float32(rope_dim)).astype(np.float32)
    inv_freq = np.power(np.float32(ROPE_THETA), expo).astype(np.float32)
    angles = np.arange(seq_len, dtype=np.float32)[:, None] * inv_freq[None, :]
    return np.cos(angles).astype(np.float32), np.sin(angles).astype(np.float32)


def rms(v, gain):
    return v * lax.rsqrt(jnp.mean(v * v, axis=-1, keepdims=True) + EPSILON) * gain


THEN = {0: (3, 5, 8), 1: (4, 6, 9), 3: (7,), 4: (10,), 5: (11,), 6: (12,), 7: (13,)}
ROUTE = 'RLDRLZZZDDDDDD'
SPLITS = ((112, 112), (112, 128), (96, 112), (32, 32), (768, 1024), (32, 32), (768, 768),
          (112, 112), (112, 112), (64, 128), (64, 64))
T_NORM, T_DOWN, T_PREP, T_ITER = 1.7, 5.2, 1.9, 2.7


def plan_transfers(pieces, steps, first):
    rate = {'R': 42e3, 'L': 42e3, 'Z': 42e3, 'D': 200e3}
    hop = {'R': 3.0, 'L': 3.0, 'Z': 3.0, 'D': 2.0}
    free = dict.fromkeys(rate, 0.0)
    state = {'now': 2.5, 'next': 0}
    arrival, done, lists = {}, set(), []

    def send(i, t):
        n, p, r, unit = pieces[i]
        pm = n - p
        size = (pm, pm, n, r, pm - r, p, p, p, pm, pm, pm, p, p, p)[t] * unit
        link = ROUTE[t]
        free[link] = max(state['now'], free[link]) + size / rate[link]
        arrival[i, t] = free[link] + hop[link]

    def own(out):
        i = state['next']
        state['next'] = i + 1
        for t in (0, 1, 2):
            send(i, t)
        out.append((i, -1))

    def wait(i, t, out):
        state['now'] = max(state['now'], arrival[i, t])
        done.add((i, t))
        out.append((i, t))
        for u in THEN.get(t, ()):
            send(i, u)

    for k, (need, busy) in enumerate(steps):
        out = []
        while True:
            while state['next'] < len(pieces) and (
                k == 0 and state['next'] < first or min(free['R'], free['L']) - state['now'] < 2
                and all((i, t) in done for i in range(first) for t in (0, 1))
            ):
                own(out)
            ready = sorted(
                (a, i, t) for (i, t), a in arrival.items()
                if (i, t) not in done and t in THEN and (t != 4 or (i, 3) in done)
            )
            if ready and ready[0][0] + 0.3 <= state['now']:
                wait(*ready[0][1:], out)
                continue
            missing = [m for m in need if m not in done]
            if not missing:
                break
            here = [m for m in missing if m in arrival and arrival[m] <= state['now']]
            if here:
                wait(*here[0], out)
                continue
            ready += [(arrival[m], *m) for m in missing if m in arrival and m[1] not in THEN]
            wait(*min(ready)[1:], out)
        lists.append(out)
        state['now'] += busy
    return lists


class Item:
    def __init__(self, index, local, full, rows, by_rows, split, col0, cols):
        self.index, self.local, self.full = index, local, full
        self.rows, self.by_rows = rows, by_rows
        self.s, self.h = split
        self.col0, self.cols = col0, cols
        self.span = rows if by_rows else cols

    def _cut(self, ref, row0, off, size):
        if self.by_rows:
            rows = pl.ds(pl.multiple_of(row0 + off, 16), size)
            cols = pl.ds(self.col0, self.cols)
        else:
            rows = pl.ds(row0 if isinstance(row0, int) else pl.multiple_of(row0, 16), self.rows)
            cols = pl.ds(pl.multiple_of(self.col0 + off, 128), size)
        return ref.at[rows, cols]

    def mine(self, off, size):
        return self._cut(self.local, 0, off, size)

    def at(self, origin, off, size):
        return self._cut(self.full, origin * self.rows, off, size)


def gather_kernel(
    dims, x_hbm, gains_hbm, wdq_l, wdkv_l, wuq_l, wukv_l, wo_l, cos_t, sin_t, cos_n, sin_n,
    o_hbm, wo_full, c_hbm, r_hbm,
    gbuf, a_s, wdq, wdkv, wdkv_t, acc_q, acc_kv, wuq, wuq_t, wukv, wk, wv_t,
    cq_t, c_s, c_t, r_s, qs, ks, vs, o_s, stage, diff_s, inv_s, gb_s, s_buf, pm, ms,
    ssem, rsem, lsem, gssem, grsem, xsem, osem, csem,
):
    n_dev, n_heads, nope, rope, vdim, d_model, q_rank, kv_rank, seq = dims
    f = lax.axis_index('fsdp')
    d = lax.axis_index('dp')
    core = lax.rem(f, 2)
    par = lax.rem(d, 2)
    chip = f // 2
    n_chip = n_dev // 2
    mod = lambda v: lax.rem(v, n_dev)
    right, left, opp = mod(f + 2), mod(f + n_dev - 2), mod(f + 4)
    partner = f + 1 - 2 * core
    p_right, p_left, p_opp = mod(partner + 2), mod(partner + n_dev - 2), mod(partner + 4)
    d_pair = d + 1 - 2 * par
    to_right, to_left, to_partner, to_pair = (d, right), (d, left), (d, partner), (d_pair, f)
    n_tok = a_s.shape[0]
    n_tile = n_tok // TILE
    half_heads = n_heads // 2
    pairs = half_heads // 2
    hd = nope + rope

    barrier = pltpu.get_barrier_semaphore()
    for step in range(1, n_dev):
        pl.semaphore_signal(barrier, inc=1, device_id=(d, mod(f + step)), device_id_type=MESH)
    pl.semaphore_signal(barrier, inc=1, device_id=to_pair, device_id_type=MESH)
    x_in = [
        pltpu.make_async_copy(x_hbm.at[pl.ds(TILE * t, TILE)], a_s.at[pl.ds(TILE * t, TILE)], xsem.at[t])
        for t in range(n_tile)
    ]
    for cp in x_in:
        cp.start()
    gain_in = pltpu.make_async_copy(gains_hbm, gbuf.at[f], lsem.at[9])
    gain_in.start()
    pl.semaphore_wait(barrier, n_dev)

    r_d, r_q, r_kv, r_o = wdq_l.shape[0], wuq_l.shape[0], wukv_l.shape[0], wo_l.shape[0]
    n_d, n_o = 2, 4
    dq_c, uq_c, ukv_c, o_c = wdq_l.shape[1] // n_d, wuq_l.shape[1] // 2, wukv_l.shape[1] // 2, wo_l.shape[1] // n_o
    parts = [(wdq_l, wdq, r_d, True, h * dq_c, dq_c) for h in range(n_d)]
    r_dkv = wdkv_l.shape[0]
    parts.append((wdkv_l, wdkv_t, r_dkv, True, 0, wdkv_l.shape[1]))
    n_down = len(parts)
    for h in range(2):
        parts.append((wuq_l, wuq, r_q, True, h * uq_c, uq_c))
        parts.append((wukv_l, wukv, r_kv, False, h * ukv_c, ukv_c))
    n_head = len(parts)
    parts += [(wo_l, wo_full, r_o, True, h * o_c, o_c) for h in range(n_o)]
    items = [Item(k, *p[:4], SPLITS[k], *p[4:]) for k, p in enumerate(parts)]

    everything = range(N_MSG)
    needs = lambda lo, hi, ts=everything: [(i, t) for i in range(lo, hi) for t in ts]
    n_pre = 7
    steps = [([], T_NORM)] * n_pre
    stages = []
    for need, cost, every in (
        (needs(0, n_down, (2,)), T_DOWN, 2),
        (needs(0, n_down, (0, 5, 8, 11)), T_DOWN, 2),
        (needs(0, n_down, (1, 6, 9, 12)), T_DOWN, 2),
        (needs(0, n_down), 1.2 * T_DOWN, 1),
    ):
        stages.append((len(steps) + 1, every))
        steps += [(need if t == 0 else [], cost * every / n_tile) for t in range(0, n_tile, every)]
    first_iter = len(steps) + 1
    for h in range(2):
        for t in range(n_tile):
            need = needs(n_down + 2 * h, n_down + 2 * h + 2) if t == 0 else []
            steps.append((need, T_ITER + (T_PREP if t == 0 else 0)))
    steps.append((needs(n_head, len(parts)), 0))
    pieces = [
        (it.span, it.s, it.h, 2 * (-(-it.cols // 128) * 128 if it.by_rows else it.rows)) for it in items
    ]
    plan = plan_transfers(pieces, [([], 0)] + steps, n_down)

    def messages(it):
        n, s, h = it.span, it.s, it.h
        own_p, pm_off, other_p = par * (n - s), par * s, (1 - par) * (n - s)
        pm, m = n - s, n - s - h
        h_off, m_off = par * (n - h), (1 - par) * h + par * s
        reg = it.at
        return [
            (it.mine(pm_off, pm), reg(f, pm_off, pm), to_right, reg(left, pm_off, pm)),
            (it.mine(pm_off, pm), reg(f, pm_off, pm), to_left, reg(right, pm_off, pm)),
            (it.mine(0, n), reg(f, 0, n), to_partner, reg(partner, 0, n)),
            (reg(left, h_off, h), reg(left, h_off, h), to_right, reg(opp, h_off, h)),
            (reg(right, m_off, m), reg(right, m_off, m), to_left, reg(opp, m_off, m)),
            (reg(left, own_p, s), reg(left, own_p, s), to_pair, reg(left, other_p, s)),
            (reg(right, own_p, s), reg(right, own_p, s), to_pair, reg(right, other_p, s)),
            (reg(opp, own_p, s), reg(opp, own_p, s), to_pair, reg(opp, other_p, s)),
            (reg(left, pm_off, pm), reg(left, pm_off, pm), to_partner, reg(p_left, pm_off, pm)),
            (reg(right, pm_off, pm), reg(right, pm_off, pm), to_partner, reg(p_right, pm_off, pm)),
            (reg(opp, pm_off, pm), reg(opp, pm_off, pm), to_partner, reg(p_opp, pm_off, pm)),
            (reg(left, other_p, s), reg(left, other_p, s), to_partner, reg(p_left, other_p, s)),
            (reg(right, other_p, s), reg(right, other_p, s), to_partner, reg(p_right, other_p, s)),
            (reg(opp, other_p, s), reg(opp, other_p, s), to_partner, reg(p_opp, other_p, s)),
        ]

    def send(it, t):
        src, dst, dev, _ = messages(it)[t]
        k = it.index * N_MSG + t
        return pltpu.make_async_remote_copy(src, dst, ssem.at[k], rsem.at[k], device_id=dev, device_id_type=MESH)

    def recv(it, t):
        _, _, dev, got = messages(it)[t]
        k = it.index * N_MSG + t
        return pltpu.make_async_remote_copy(got, got, ssem.at[k], rsem.at[k], device_id=dev, device_id_type=MESH)

    def start(it, *ts):
        for t in ts:
            send(it, t).start()

    def got(it, *ts):
        for t in ts:
            recv(it, t).wait_recv()

    def local_copy(it):
        return pltpu.make_async_copy(it.mine(0, it.span), it.at(f, 0, it.span), lsem.at[it.index])

    stage_in = pltpu.make_async_copy(wo_l, stage, lsem.at[n_head])
    stage_out = pltpu.make_async_copy(stage, wo_full.at[pl.ds(pl.multiple_of(f * r_o, 16), r_o)], lsem.at[n_head + 1])

    def pump(segment):
        for i, t in segment:
            it = items[i]
            if t < 0:
                start(it, 0, 1, 2)
                if i < n_head:
                    local_copy(it).start()
            else:
                got(it, t)
                start(it, *THEN.get(t, ()))

    def own_rows(first, last):
        for i in range(first, last):
            local_copy(items[i]).wait()

    def gain_copy(step):
        return pltpu.make_async_remote_copy(
            gbuf.at[f], gbuf.at[f], gssem.at[step - 1], grsem.at[step - 1],
            device_id=(d, mod(f + step)), device_id_type=MESH,
        )

    gain_in.wait()
    for step in range(1, n_dev):
        gain_copy(step).start()
    pump(plan[0])
    stage_in.start()

    row_i = lax.broadcasted_iota(jnp.int32, (seq, 2 * seq), 0)
    lane_i = lax.broadcasted_iota(jnp.int32, (seq, 2 * seq), 1)
    diff_s[...] = lax.rem(lane_i, seq) - row_i
    for p in range(2):
        @pl.loop(0, pairs)
        def _(j, p=p):
            qs[p, j] = jnp.zeros(qs.shape[2:], BF16)

    @pl.loop(0, pairs)
    def _(j):
        for b in range(2):
            vs[b, j, :2 * vdim, :] = jnp.zeros((2 * vdim, vs.shape[3]), BF16)
            vs[b, j, 2 * vdim:, :] = jnp.ones((vs.shape[2] - 2 * vdim, vs.shape[3]), BF16)
        s_buf[1, j] = jnp.zeros(s_buf.shape[2:], F32)

    r_s[...] = jnp.zeros(r_s.shape, BF16)
    ms[...] = jnp.zeros(ms.shape, F32)

    for t, cp in enumerate(x_in):
        if t in (n_tile // 2, 3 * n_tile // 4):
            pump(plan[1 if t == n_tile // 2 else 2])
        cp.wait()
        v = a_s[TILE * t:TILE * (t + 1), :].astype(F32)
        inv_s[TILE * t:TILE * (t + 1), :] = lax.rsqrt(jnp.mean(v * v, axis=-1, keepdims=True) + EPSILON)

    for step in range(1, n_dev):
        gain_copy(step).wait_recv()
    n_in, n_q, n_kv = d_model // n_dev, q_rank // n_dev, kv_rank // n_dev
    join = lambda lo, n: jnp.concatenate([gbuf[i][:, lo:lo + n] for i in range(n_dev)], axis=1)
    g_in, g_q, g_kv = join(0, n_in), join(n_in, n_q), join(n_in + n_q, n_kv)

    gb_s[...] = jnp.broadcast_to(g_in, gb_s.shape)
    pump(plan[3])
    n_norm = n_tok // NORM

    @pl.loop(0, n_norm)
    def _(t):
        for k in range(1, 4):
            @pl.when(t == k * n_norm // 4)
            def _(k=k):
                pump(plan[3 + k])
        rows = pl.ds(pl.multiple_of(t * NORM, NORM), NORM)
        v = a_s[rows, :].astype(F32) * inv_s[rows, :]
        v = v.reshape(NORM // 8, 8, d_model) * gb_s[...][None]
        a_s[rows, :] = v.reshape(NORM, d_model).astype(BF16)

    pump(plan[n_pre])

    depth = 2 * r_d

    chip_cols = lambda c: pl.ds(pl.multiple_of(lax.rem(chip + c, n_chip) * depth, 128), depth)
    tile_rows = lambda t: pl.ds(pl.multiple_of(t * TILE, TILE), TILE)

    def down(t, hops):
        rows = tile_rows(t)
        cols = [chip_cols(c) for c in hops]
        a = jnp.concatenate([a_s[rows, c] for c in cols], axis=1)
        for w, acc in ((wdq, acc_q), (wdkv, acc_kv)):
            part = jnp.dot(a, jnp.concatenate([w[c, :] for c in cols], axis=0), preferred_element_type=F32)
            if hops[0] == 0:
                acc[rows, :] = part
            else:
                acc[rows, :] += part

    def turn(hops):
        for c in hops:
            for k in range(2):
                origin = lax.rem(chip + c, n_chip) * 2 + k
                block = wdkv_t[pl.ds(pl.multiple_of(origin * r_dkv, 16), r_dkv), :]
                wdkv[pl.ds(pl.multiple_of(origin * r_d, 16), r_d), :] = block.T

    def finish(t):
        rows = tile_rows(t)
        cq_t[:, rows] = rms(acc_q[rows, :], g_q).astype(BF16).T
        kv = acc_kv[rows, :]
        lat = rms(kv[:, :kv_rank], g_kv).astype(BF16)
        c_s[rows, :] = lat
        c_t[:, rows] = lat.T
        pe = kv[:, kv_rank:]
        swapped = jnp.concatenate([pe[:, rope // 2:], pe[:, :rope // 2]], axis=1)
        r_s[rows, :rope] = (pe * cos_n[...] + swapped * sin_n[...]).astype(BF16)

    own_rows(0, n_down)
    def look(stage, t):
        base, every = stages[stage]
        for q in range(1, n_tile // every):
            if plan[base + q]:
                @pl.when(t == q * every)
                def _(q=q):
                    pump(plan[base + q])

    for k, hops in enumerate(((0,), (n_chip - 1,), (1,))):
        pump(plan[stages[k][0]])
        turn(hops)

        @pl.loop(0, n_tile)
        def _(t):
            look(k, t)
            down(t, hops)

    pump(plan[stages[3][0]])
    turn((2,))
    down(0, (2,))

    @pl.loop(1, n_tile)
    def _(t):
        look(3, t)
        down(t, (2,))
        finish(t - 1)

    finish(n_tile - 1)
    stage_in.wait()
    stage_out.start()
    c_out = pltpu.make_async_copy(c_s, c_hbm, csem.at[0])
    r_out = pltpu.make_async_copy(r_s, r_hbm, csem.at[1])
    c_out.start()
    r_out.start()

    scale = float((nope + rope) ** -0.5)
    exp_scale = scale * float(np.log2(np.e))
    fill = -1e30 / scale
    cos_q, sin_q = cos_t[...], sin_t[...]
    hr = rope // 2

    def o_copy(it):
        h, t, slot = it // n_tile, it % n_tile, it % 3
        return pltpu.make_async_copy(
            o_s.at[slot],
            o_hbm.at[pl.ds(pl.multiple_of(t * TILE, TILE), TILE),
                     pl.ds(pl.multiple_of(h * half_heads * vdim, 128), half_heads * vdim)],
            osem.at[slot],
        )

    groups = seq // 8

    def maxima(p):
        for side in range(2):
            base = 16 * pairs * side + 8 * pairs * p
            part = [pm[pl.ds(base + i, pairs, stride=8), :] for i in range(8)]
            ms[pairs * p:pairs * (p + 1), seq * side:seq * (side + 1)] = functools.reduce(jnp.maximum, part)

    def values(p, j, slot, o_slot):
        k = p * pairs + j
        m = jnp.broadcast_to(ms[k:k + 1, :], (8, 2 * seq))
        s = s_buf[p, j].reshape(groups, 8, 2 * seq)
        e = jnp.exp2((s - m[None]) * exp_scale).astype(BF16).reshape(seq, 2 * seq)
        ov = jnp.dot(vs[slot, j, :, seq * p:seq * (p + 1)], e, preferred_element_type=F32)
        inv = (1.0 / ov[2 * vdim:2 * vdim + 8, :])[None]
        oa = ov[:vdim, :seq].reshape(vdim // 8, 8, seq) * inv[:, :, :seq]
        ob = ov[vdim:2 * vdim, seq:].reshape(vdim // 8, 8, seq) * inv[:, :, seq:]
        o_t = jnp.concatenate([oa, ob], axis=0).reshape(2 * vdim, seq).astype(BF16)
        o_s[o_slot, seq * p:seq * (p + 1), 2 * vdim * j:2 * vdim * (j + 1)] = o_t.T

    chunk = 4

    @pl.loop(0, 2)
    def _(h):
        for k in range(2):
            @pl.when(h == k)
            def _(k=k):
                pump(plan[first_iter + k * n_tile])
                own_rows(n_down + 2 * k, n_down + 2 * k + 2)
        for b in range(uq_c // 128):
            cols = pl.ds(pl.multiple_of(h * uq_c + b * 128, 128), 128)
            wuq_t[b * 128:(b + 1) * 128, :] = wuq[:, cols].T
        for j in range(pairs):
            c0 = h * ukv_c + j * 2 * (nope + vdim)
            wa = wukv[:, pl.ds(pl.multiple_of(c0, 128), nope + vdim)]
            wb = wukv[:, pl.ds(pl.multiple_of(c0 + nope + vdim, 128), nope + vdim)]
            wk[:, 2 * nope * j:2 * nope * (j + 1)] = jnp.concatenate([wa[:, :nope], wb[:, :nope]], axis=1)
            wv_t[2 * vdim * j:2 * vdim * (j + 1), :] = jnp.concatenate([wa.T[nope:], wb.T[nope:]], axis=0)

        @pl.loop(0, n_tile)
        def _(t):
            it = h * n_tile + t
            for q in range(4):
                @pl.when(it // (n_tile // 2) == q)
                def _(q=q):
                    for k in range(q * n_tile // 2, (q + 1) * n_tile // 2):
                        if k % n_tile and plan[first_iter + k]:
                            @pl.when(it == k)
                            def _(k=k):
                                pump(plan[first_iter + k])

            @pl.when(it >= 3)
            def _():
                o_copy(it - 3).wait()

            @pl.when(it >= 2)
            def _():
                o_copy(it - 2).start()

            slot = lax.rem(it, 2)
            rows = pl.ds(pl.multiple_of(t * TILE, TILE), TILE)
            cq = cq_t[:, rows]
            for g in range(half_heads // chunk):
                w = wuq_t[g * chunk * hd:(g + 1) * chunk * hd, :]
                q = jnp.dot(w, cq, preferred_element_type=F32)
                for hh in range(chunk):
                    j, side = (g * chunk + hh) // 2, hh % 2
                    r0 = hh * hd
                    for p in range(2):
                        lanes = slice(seq * p, seq * (p + 1))
                        dst = slice(seq * side, seq * (side + 1))
                        qs[p, j, side * nope:(side + 1) * nope, dst] = q[r0:r0 + nope, lanes].astype(BF16)
                        lo = q[r0 + nope:r0 + nope + hr, lanes]
                        hi = q[r0 + nope + hr:r0 + hd, lanes]
                        qs[p, j, 2 * nope:2 * nope + hr, dst] = (lo * cos_q - hi * sin_q).astype(BF16)
                        qs[p, j, 2 * nope + hr:2 * nope + rope, dst] = (hi * cos_q + lo * sin_q).astype(BF16)
            lat = c_s[rows, :]
            ks[...] = jnp.dot(lat, wk[...], preferred_element_type=F32).astype(BF16)
            v = jnp.dot(wv_t[...], c_t[:, rows], preferred_element_type=F32).astype(BF16)
            for j in range(pairs):
                vs[slot, j, :2 * vdim, :] = v[2 * vdim * j:2 * vdim * (j + 1)]

            r_blk = [r_s[pl.ds(pl.multiple_of(t * TILE + p * seq, seq), seq), :] for p in range(2)]
            def scores(p, j):
                lhs = jnp.concatenate([ks[seq * p:seq * (p + 1), 2 * nope * j:2 * nope * (j + 1)], r_blk[p]], axis=1)
                s = jnp.dot(lhs, qs[p, j], preferred_element_type=F32)
                s = jnp.where(diff_s[...] >= 0, s, fill)
                s_buf[p, j] = s
                k = p * pairs + j
                top = jnp.max(s.reshape(groups, 8, 2 * seq), axis=0)
                pm[8 * k:8 * (k + 1), :] = top[:, :seq]
                pm[16 * pairs + 8 * k:16 * pairs + 8 * (k + 1), :] = top[:, seq:]

            for j in range(pairs):
                scores(0, j)
                values(1, j, 1 - slot, lax.rem(it + 2, 3))
            maxima(0)

            for j in range(pairs):
                scores(1, j)
                values(0, j, slot, lax.rem(it, 3))
            maxima(1)

    last = 2 * n_tile - 1
    o_copy(last - 2).wait()
    o_copy(last - 1).start()
    for j in range(pairs):
        values(1, j, last % 2, last % 3)
    o_copy(last).start()

    pump(plan[first_iter + 2 * n_tile])
    stage_out.wait()
    o_copy(last - 1).wait()
    o_copy(last).wait()
    c_out.wait()
    r_out.wait()
    for step in range(1, n_dev):
        gain_copy(step).wait_send()
    for it in items:
        for t in range(N_MSG):
            send(it, t).wait_send()


def out_kernel(o_ref, w_ref, x_ref, c_ref, r_ref, y_ref, c_out, r_out):
    acc = jnp.dot(o_ref[...], w_ref[...], preferred_element_type=F32)
    y_ref[...] = (x_ref[...].astype(F32) + acc).astype(BF16)
    c_out[...] = c_ref[...]
    seq = r_out.shape[2]
    for p in range(r_out.shape[0]):
        r_out[p] = r_ref[p * seq:(p + 1) * seq, :].T[:r_out.shape[1]]


def solution(mesh):
    batch_spec = P(('dp', 'fsdp'))
    row_spec = P('fsdp')
    mat_spec = P('fsdp', None)
    n_dev = mesh.shape['fsdp']
    assert n_dev == 8 and mesh.shape['dp'] % 2 == 0

    def local_block(tok, g_in, w_dq, g_q, w_uq, w_dkv, g_kv, w_ukv, w_out):
        n_p, seq, d_model = tok.shape
        n_tok = n_p * seq
        kv_rank, q_rank = g_kv.shape[0] * n_dev, g_q.shape[0] * n_dev
        rope = w_dkv.shape[1] - kv_rank
        nope_total = w_ukv.shape[1] - w_out.shape[0] * n_dev
        n_heads = (w_uq.shape[1] - nope_total) // rope
        nope = nope_total // n_heads
        vdim = w_out.shape[0] * n_dev // n_heads
        pairs = n_heads // 4
        hh = n_heads // 2
        x2 = tok.reshape(n_tok, d_model)
        gains = jnp.concatenate([g_in, g_q, g_kv]).astype(F32)
        gains = jnp.pad(gains, (0, -gains.shape[0] % 128))[None]
        cos, sin = rope_tables(seq, rope)
        cos_t, sin_t = jnp.asarray(cos.T), jnp.asarray(sin.T)
        reps = TILE // seq
        cos_n = jnp.asarray(np.tile(np.concatenate([cos, cos], 1), (reps, 1)))
        sin_n = jnp.asarray(np.tile(np.concatenate([-sin, sin], 1), (reps, 1)))
        dims = (n_dev, n_heads, nope, rope, vdim, d_model, q_rank, kv_rank, seq)
        n_items = len(SPLITS)
        any_ = pl.BlockSpec(memory_space=pl.ANY)
        vm = pl.BlockSpec(memory_space=pltpu.VMEM)
        o, wo_full, c_all, r_all = pl.pallas_call(
            functools.partial(gather_kernel, dims),
            out_shape=(
                jax.ShapeDtypeStruct((n_tok, n_heads * vdim), BF16),
                jax.ShapeDtypeStruct((n_heads * vdim, d_model), BF16),
                jax.ShapeDtypeStruct((n_tok, kv_rank), BF16),
                jax.ShapeDtypeStruct((n_tok, 128), BF16),
            ),
            in_specs=[any_] * 7 + [vm] * 4,
            out_specs=(any_,) * 4,
            scratch_shapes=[
                pltpu.VMEM((n_dev, 1, gains.shape[1]), F32),
                pltpu.VMEM((n_tok, d_model), BF16),
                pltpu.VMEM((d_model, q_rank), BF16),
                pltpu.VMEM((d_model, kv_rank + rope), BF16),
                pltpu.VMEM((n_dev * w_dkv.shape[1], w_dkv.shape[0]), BF16),
                pltpu.VMEM((n_tok, q_rank), F32),
                pltpu.VMEM((n_tok, kv_rank + rope), F32),
                pltpu.VMEM((q_rank, w_uq.shape[1]), BF16),
                pltpu.VMEM((w_uq.shape[1] // 2, q_rank), BF16),
                pltpu.VMEM((kv_rank, w_ukv.shape[1]), BF16),
                pltpu.VMEM((kv_rank, hh * nope), BF16),
                pltpu.VMEM((hh * vdim, kv_rank), BF16),
                pltpu.VMEM((q_rank, n_tok), BF16),
                pltpu.VMEM((n_tok, kv_rank), BF16),
                pltpu.VMEM((kv_rank, n_tok), BF16),
                pltpu.VMEM((n_tok, 128), BF16),
                pltpu.VMEM((2, pairs, 2 * nope + 128, 2 * seq), BF16),
                pltpu.VMEM((TILE, hh * nope), BF16),
                pltpu.VMEM((2, pairs, 2 * vdim + 16, TILE), BF16),
                pltpu.VMEM((3, TILE, hh * vdim), BF16),
                pltpu.VMEM(w_out.shape, BF16),
                pltpu.VMEM((seq, 2 * seq), jnp.int32),
                pltpu.VMEM((n_tok, 1), F32),
                pltpu.VMEM((8, d_model), F32),
                pltpu.VMEM((2, pairs, seq, 2 * seq), F32),
                pltpu.VMEM((2 * 2 * pairs * 8, seq), F32),
                pltpu.VMEM((2 * pairs, 2 * seq), F32),
                pltpu.SemaphoreType.DMA((n_items * N_MSG,)),
                pltpu.SemaphoreType.DMA((n_items * N_MSG,)),
                pltpu.SemaphoreType.DMA((10,)),
                pltpu.SemaphoreType.DMA((n_dev - 1,)),
                pltpu.SemaphoreType.DMA((n_dev - 1,)),
                pltpu.SemaphoreType.DMA((n_tok // TILE,)),
                pltpu.SemaphoreType.DMA((3,)),
                pltpu.SemaphoreType.DMA((2,)),
            ],
            compiler_params=pltpu.CompilerParams(
                collective_id=0, has_side_effects=True, vmem_limit_bytes=67_043_328,
            ),
            name='gather_attend',
        )(x2, gains, w_dq, w_dkv.T, w_uq, w_ukv, w_out, cos_t, sin_t, cos_n, sin_n)

        bm, bn = 512, 1280
        n_m, n_n = n_tok // bm, d_model // bn
        once = lambda n, m: (jnp.where(n == 0, m, n_m - 1), 0)
        y, c_blk, r_blk = pl.pallas_call(
            out_kernel,
            grid=(n_n, n_m),
            in_specs=[
                pl.BlockSpec((bm, n_heads * vdim), lambda n, m: (m, 0)),
                pl.BlockSpec((n_heads * vdim, bn), lambda n, m: (0, n)),
                pl.BlockSpec((bm, bn), lambda n, m: (m, n)),
                pl.BlockSpec((bm, kv_rank), once),
                pl.BlockSpec((bm, 128), once),
            ],
            out_specs=[
                pl.BlockSpec((bm, bn), lambda n, m: (m, n)),
                pl.BlockSpec((bm, kv_rank), once),
                pl.BlockSpec((bm // seq, rope, seq), lambda n, m: (jnp.where(n == 0, m, n_m - 1), 0, 0)),
            ],
            out_shape=[
                jax.ShapeDtypeStruct((n_tok, d_model), BF16),
                jax.ShapeDtypeStruct((n_tok, kv_rank), BF16),
                jax.ShapeDtypeStruct((n_p, rope, seq), BF16),
            ],
            compiler_params=pltpu.CompilerParams(vmem_limit_bytes=60 * 1024 * 1024),
            name='project_out',
        )(o, wo_full, x2, c_all, r_all)
        return y.reshape(tok.shape), c_blk.reshape(n_p, seq, kv_rank), jnp.swapaxes(r_blk, 1, 2)

    return jax.shard_map(
        local_block,
        mesh=mesh,
        in_specs=(batch_spec, row_spec, mat_spec, row_spec, mat_spec, mat_spec, row_spec, mat_spec, mat_spec),
        out_specs=(batch_spec, batch_spec, batch_spec),
        check_vma=False,
    )
```
